32 devices in a mesh: dp: 4 (over y, z), sp: 8 (over x, core).
Axes of the slice: x: 4, y: 2, z: 2, core: 2. Of those that a mesh axis runs over, the one named last changes fastest.
The devices are a block of a 4x4x8 slice.
Arguments:
- hidden_in: bfloat16 [32768, 1152], P(('dp', 'sp')), parts along dimension 0
- w_query: bfloat16 [1152, 4, 256], replicated
- w_key: bfloat16 [1152, 1, 256], replicated
- w_value: bfloat16 [1152, 1, 256], replicated
- w_out: bfloat16 [4, 256, 1152], replicated
- w_up: bfloat16 [1152, 6912], replicated
- w_down: bfloat16 [6912, 1152], replicated
- rel_bias: float32 [4, 1025], replicated
- glob_pos: int32 [1024], P('dp'), parts along dimension 0
Outputs:
- output 1: bfloat16 [32768, 1152], P(('dp', 'sp')), parts along dimension 0
- output 2: bfloat16 [1024, 1152], P('dp'), parts along dimension 0
There are 4 independent parts. The reference program is written for one: setup_inputs(seed, part) draws one part's arguments, and reference() takes and returns one part's arrays. A program takes and returns all parts, laid end to end along the dimension named above; an argument that names none is the same for every part.
All inputs are finite; a program needn't handle non-finite values.
Results may differ from the reference program's by a relative error of at most 0.00839907.
Values are sent between devices in bfloat16 or wider.
A program may use at most 768 MiB of HBM per device.

```python
import jax
import jax.numpy as jnp
from jax import lax

SEQ_LEN = 8192
MODEL_DIM = 1152
QUERY_HEADS = 4
KV_HEADS = 1
HEAD_DIM = 256
FFN_DIM = 6912
WINDOW = 512
GLOBAL_TOKENS = 256
ROW_SPAN = 1024


def draw_positions(key):
    inner = jax.random.permutation(key, SEQ_LEN - 2)[: GLOBAL_TOKENS - 2] + 1
    ends = jnp.array([0, SEQ_LEN - 1], dtype=jnp.int32)
    return jnp.sort(jnp.concatenate([ends, inner.astype(jnp.int32)]))


def setup_inputs(seed: int = 0, part: int = 0) -> dict:
    shared = jax.random.key(seed)
    part_key = jax.random.fold_in(shared, part)
    weight_keys = jax.random.split(shared, 8)
    qk_scale = 1.7 * MODEL_DIM ** -0.5
    hidden_in = jax.random.normal(jax.random.fold_in(part_key, 1), (SEQ_LEN, MODEL_DIM), jnp.float32)
    w_query = jax.random.normal(weight_keys[0], (MODEL_DIM, QUERY_HEADS, HEAD_DIM), jnp.float32) * qk_scale
    w_key = jax.random.normal(weight_keys[1], (MODEL_DIM, KV_HEADS, HEAD_DIM), jnp.float32) * qk_scale
    w_value = jax.random.normal(weight_keys[2], (MODEL_DIM, KV_HEADS, HEAD_DIM), jnp.float32) * MODEL_DIM ** -0.5
    w_out = jax.random.normal(weight_keys[3], (QUERY_HEADS, HEAD_DIM, MODEL_DIM), jnp.float32) * (QUERY_HEADS * HEAD_DIM) ** -0.5
    w_up = jax.random.normal(weight_keys[4], (MODEL_DIM, FFN_DIM), jnp.float32) * MODEL_DIM ** -0.5
    w_down = jax.random.normal(weight_keys[5], (FFN_DIM, MODEL_DIM), jnp.float32) * FFN_DIM ** -0.5
    rel_bias = jax.random.normal(weight_keys[6], (QUERY_HEADS, 2 * WINDOW + 1), jnp.float32)
    glob_pos = draw_positions(jax.random.fold_in(part_key, 2))
    return {
        'hidden_in': hidden_in.astype(jnp.bfloat16),
        'w_query': w_query.astype(jnp.bfloat16),
        'w_key': w_key.astype(jnp.bfloat16),
        'w_value': w_value.astype(jnp.bfloat16),
        'w_out': w_out.astype(jnp.bfloat16),
        'w_up': w_up.astype(jnp.bfloat16),
        'w_down': w_down.astype(jnp.bfloat16),
        'rel_bias': rel_bias,
        'glob_pos': glob_pos,
    }


def reference(hidden_in, w_query, w_key, w_value, w_out, w_up, w_down, rel_bias, glob_pos):
    group = QUERY_HEADS // KV_HEADS
    n_blocks = ROW_SPAN // WINDOW
    queries = (jnp.dot(hidden_in, w_query.reshape(MODEL_DIM, QUERY_HEADS * HEAD_DIM), preferred_element_type=jnp.float32) * HEAD_DIM ** -0.5).astype(jnp.bfloat16)
    keys_all = jnp.dot(hidden_in, w_key.reshape(MODEL_DIM, KV_HEADS * HEAD_DIM), preferred_element_type=jnp.float32).astype(jnp.bfloat16)
    vals_all = jnp.dot(hidden_in, w_value.reshape(MODEL_DIM, KV_HEADS * HEAD_DIM), preferred_element_type=jnp.float32).astype(jnp.bfloat16)
    queries = queries.reshape(SEQ_LEN, KV_HEADS, group, HEAD_DIM).astype(jnp.float32)
    keys_all = keys_all.reshape(SEQ_LEN, KV_HEADS, HEAD_DIM).astype(jnp.float32)
    vals_all = vals_all.reshape(SEQ_LEN, KV_HEADS, HEAD_DIM).astype(jnp.float32)
    glob_flag = jnp.zeros((SEQ_LEN,), jnp.int32).at[glob_pos].set(1)
    key_ok_pad = jnp.pad(1 - glob_flag, (WINDOW, WINDOW)) > 0
    keys_pad = jnp.pad(keys_all, ((WINDOW, WINDOW), (0, 0), (0, 0)))
    vals_pad = jnp.pad(vals_all, ((WINDOW, WINDOW), (0, 0), (0, 0)))
    key_glob = keys_all[glob_pos]
    val_glob = vals_all[glob_pos]
    row_idx = jnp.arange(WINDOW)[:, None]
    col_idx = jnp.arange(3 * WINDOW)[None, :]
    band = jnp.abs(col_idx - row_idx - WINDOW) <= WINDOW
    bias = jnp.take(rel_bias, jnp.clip(col_idx - row_idx, 0, 2 * WINDOW), axis=1).reshape(KV_HEADS, group, WINDOW, 3 * WINDOW)

    def three_blocks(ext):
        blocks = ext.reshape((n_blocks + 2, WINDOW) + ext.shape[1:])
        return jnp.concatenate([blocks[:-2], blocks[1:-1], blocks[2:]], axis=1)

    def span_attention(start):
        query_blk = lax.dynamic_slice_in_dim(queries, start, ROW_SPAN, 0).reshape(n_blocks, WINDOW, KV_HEADS, group, HEAD_DIM)
        key_win = three_blocks(lax.dynamic_slice_in_dim(keys_pad, start, ROW_SPAN + 2 * WINDOW, 0))
        val_win = three_blocks(lax.dynamic_slice_in_dim(vals_pad, start, ROW_SPAN + 2 * WINDOW, 0))
        ok_win = three_blocks(lax.dynamic_slice_in_dim(key_ok_pad, start, ROW_SPAN + 2 * WINDOW, 0))
        mask = band & ok_win[:, None, None, None, :]
        score_win = jnp.where(mask, jnp.einsum('bqgrd,bkgd->bgrqk', query_blk, key_win) + bias, -1e30)
        score_glob = jnp.einsum('bqgrd,ngd->bgrqn', query_blk, key_glob)
        top = jnp.maximum(score_win.max(-1), score_glob.max(-1))[..., None]
        prob_win = jnp.exp(score_win - top)
        prob_glob = jnp.exp(score_glob - top)
        norm_sum = prob_win.sum(-1) + prob_glob.sum(-1)
        weighted = jnp.einsum('bgrqk,bkgd->bgrqd', prob_win.astype(jnp.bfloat16).astype(jnp.float32), val_win)
        weighted = weighted + jnp.einsum('bgrqn,ngd->bgrqd', prob_glob.astype(jnp.bfloat16).astype(jnp.float32), val_glob)
        result = weighted / norm_sum[..., None]
        return jnp.transpose(result, (0, 3, 1, 2, 4)).reshape(ROW_SPAN, QUERY_HEADS * HEAD_DIM)

    starts = jnp.arange(SEQ_LEN // ROW_SPAN) * ROW_SPAN
    attended = lax.map(span_attention, starts).reshape(SEQ_LEN, QUERY_HEADS * HEAD_DIM)
    query_glob = queries[glob_pos]
    score_full = jnp.einsum('ngrd,tgd->ngrt', query_glob, keys_all)
    prob_full = jnp.exp(score_full - score_full.max(-1, keepdims=True))
    out_glob = jnp.einsum('ngrt,tgd->ngrd', prob_full.astype(jnp.bfloat16).astype(jnp.float32), vals_all) / prob_full.sum(-1)[..., None]
    attended = attended.at[glob_pos].set(out_glob.reshape(GLOBAL_TOKENS, QUERY_HEADS * HEAD_DIM)).astype(jnp.bfloat16)
    hidden = (hidden_in.astype(jnp.float32) + jnp.dot(attended, w_out.reshape(QUERY_HEADS * HEAD_DIM, MODEL_DIM), preferred_element_type=jnp.float32)).astype(jnp.bfloat16)
    upper = jax.nn.gelu(jnp.dot(hidden, w_up, preferred_element_type=jnp.float32)).astype(jnp.bfloat16)
    y_out = (hidden.astype(jnp.float32) + jnp.dot(upper, w_down, preferred_element_type=jnp.float32)).astype(jnp.bfloat16)
    return y_out, y_out[glob_pos]
```

```python
import functools

import jax
import jax.numpy as jnp
from jax import lax
from jax.experimental import pallas as pl
from jax.experimental.pallas import tpu as pltpu
from jax.sharding import PartitionSpec as P

MESH = pl.DeviceIdType.MESH
F32 = jnp.float32
BF16 = jnp.bfloat16
QB = 128
VMEM_LIMIT = 60 * 1024 * 1024


def mm(a, b):
    return jnp.dot(a, b, preferred_element_type=F32)


def mm_ta(a, b):
    return lax.dot_general(a, b, (((0,), (0,)), ((), ())), preferred_element_type=F32)


def mm_tb(a, b):
    return lax.dot_general(a, b, (((1,), (1,)), ((), ())), preferred_element_type=F32)


def send(src, dst, ssem, rsem, dev):
    copy = pltpu.make_async_remote_copy(
        src_ref=src, dst_ref=dst, send_sem=ssem, recv_sem=rsem, device_id={'sp': dev}, device_id_type=MESH)
    copy.start()
    return copy


def arrival(ref, ssem, rsem, dev):
    return pltpu.make_async_remote_copy(
        src_ref=ref, dst_ref=ref, send_sem=ssem, recv_sem=rsem, device_id={'sp': dev}, device_id_type=MESH)


def greet(sp):
    me = lax.axis_index('sp')
    barrier = pltpu.get_barrier_semaphore()
    for k in range(1, sp):
        pl.semaphore_signal(barrier, inc=1, device_id={'sp': lax.rem(me + k, sp)}, device_id_type=MESH)
    return barrier


def gather_blocks(buf, chips, chip, core, ssem, rsem):
    sends = []
    mine = buf.at[core * chips + chip]
    for k in range(1, chips):
        peer = lax.rem(chip + k, chips) * 2 + core
        sends.append(send(mine, mine, ssem.at[k], rsem.at[k], peer))
    return sends


def gather_forward(buf, chips, chip, core, ssem, rsem):
    partner = chip * 2 + 1 - core
    for k in range(1, chips):
        src = lax.rem(chip - k + chips, chips)
        arrival(buf.at[core * chips + src], ssem.at[k], rsem.at[k], partner).wait_recv()
    half = buf.at[pl.ds(core * chips, chips)]
    return send(half, half, ssem.at[0], rsem.at[0], partner)


def gather_finish(buf, chips, chip, core, ssem, rsem, sends):
    partner = chip * 2 + 1 - core
    other = buf.at[pl.ds((1 - core) * chips, chips)]
    arrival(other, ssem.at[0], rsem.at[0], partner).wait_recv()
    for copy in sends:
        copy.wait_send()


def attention_kernel(sp, heads, x_hbm, wq_hbm, wk_hbm, wv_hbm, wo_hbm, rel_ref, gp_ref, h_ref,
                     x_ref, wq_ref, wk_ref, wv_ref, wo_ref, rel_pad, tile, onehot, kmask,
                     kt, kloc, vt, vext, qs, qg, ktg, vg, att,
                     xp, xq, xs, xr, xg, part, pq, pc, pr,
                     load_sem, halo_s, halo_r, pick_s, pick_r, xg_s, xg_r, part_s, part_r):
    me = lax.axis_index('sp')
    chips = sp // 2
    chip, core = me // 2, lax.rem(me, 2)
    partner = chip * 2 + 1 - core
    rows, dim = x_ref.shape
    head = wk_ref.shape[1]
    width = (rel_ref.shape[1] - 1) // 2
    span = 2 * width + QB
    n_glob = gp_ref.shape[1]
    share = n_glob // sp
    ext = rows + 2 * width
    seq = rows * sp
    start = me * rows
    ninf = -jnp.inf

    loads = []
    for i, (src, dst) in enumerate(((x_hbm, x_ref), (wk_hbm, wk_ref), (wv_hbm, wv_ref), (wq_hbm, wq_ref), (wo_hbm, wo_ref))):
        copy = pltpu.make_async_copy(src, dst, load_sem.at[i])
        copy.start()
        loads.append(copy)
    barrier = greet(sp)

    pos = start - width + lax.broadcasted_iota(jnp.int32, (ext, n_glob), 0)
    onehot[...] = jnp.where(pos == gp_ref[...], 1.0, 0.0).astype(BF16)
    count = mm_tb(jnp.ones((8, n_glob), BF16), onehot[...])[0:1]
    col = start - width + lax.broadcasted_iota(jnp.int32, (1, ext), 1)
    kmask[...] = jnp.where((count > 0.5) | (col < 0) | (col >= seq), ninf, 0.0)
    rel_pad[...] = jnp.full(rel_pad.shape, ninf, F32)
    rel_pad[:, : 2 * width + 1] = rel_ref[...]
    for h in range(heads):
        line = jnp.broadcast_to(rel_pad[h : h + 1, :], (QB, span))
        tile[h * QB : (h + 1) * QB, :] = pltpu.roll(line, 0, 1, stride=1, stride_axis=0)

    loads[0].wait()
    own = onehot[width : width + rows, :]
    picked = mm_ta(own, x_ref[...]).astype(BF16)
    xp[...] = picked.reshape(xp.shape)
    pl.semaphore_wait(barrier, sp - 1)
    pick_send = [send(xp.at[1 - core], xq, pick_s.at[0], pick_r.at[0], partner)]

    loads[1].wait()
    loads[2].wait()
    k32 = mm(x_ref[...], wk_ref[...])
    kloc[...] = k32.astype(BF16)
    kt[:, width : width + rows] = k32.T.astype(BF16)
    v32 = mm(x_ref[...], wv_ref[...])
    vext[width : width + rows, :] = v32.astype(BF16)
    vt[...] = v32.T.astype(BF16)
    right, left = lax.rem(me + 1, sp), lax.rem(me + sp - 1, sp)
    halo = [
        send(kt.at[:, pl.ds(rows, width)], kt.at[:, pl.ds(0, width)], halo_s.at[0], halo_r.at[0], right),
        send(vext.at[pl.ds(rows, width)], vext.at[pl.ds(0, width)], halo_s.at[1], halo_r.at[1], right),
        send(kt.at[:, pl.ds(width, width)], kt.at[:, pl.ds(width + rows, width)], halo_s.at[2], halo_r.at[2], left),
        send(vext.at[pl.ds(width, width)], vext.at[pl.ds(width + rows, width)], halo_s.at[3], halo_r.at[3], left),
    ]

    arrival(xq, pick_s.at[0], pick_r.at[0], partner).wait_recv()
    xs[...] = xp[core] + xq[...]
    for k in range(1, chips):
        there = lax.rem(chip + k, chips)
        pick_send.append(send(xs.at[there], xr.at[k - 1], pick_s.at[k], pick_r.at[k], there * 2 + core))

    loads[3].wait()
    scale = head ** -0.5

    def project(b, carry):
        xb = x_ref[pl.ds(b * 2 * QB, 2 * QB), :]
        qb = (mm(xb, wq_ref[...]) * scale).astype(BF16)
        for r in range(2):
            for h in range(heads):
                qs[2 * b + r, h * QB : (h + 1) * QB, :] = qb[r * QB : (r + 1) * QB, h * head : (h + 1) * head]
        return carry

    lax.fori_loop(0, rows // (2 * QB), project, 0)

    for k in range(1, chips):
        arrival(xr.at[k - 1], pick_s.at[k], pick_r.at[k], partner).wait_recv()
    mine = xs[chip]
    for k in range(1, chips):
        mine = mine + xr[k - 1]
    xg[core * chips + chip] = mine
    xg_send = gather_blocks(xg, chips, chip, core, xg_s, xg_r)
    for copy in pick_send:
        copy.wait_send()
    xg_send.append(gather_forward(xg, chips, chip, core, xg_s, xg_r))
    gather_finish(xg, chips, chip, core, xg_s, xg_r, xg_send)

    xgv = xg[...].reshape(n_glob, dim)
    qgv = (mm(xgv, wq_ref[...]) * scale).astype(BF16)
    ktg[...] = mm(xgv, wk_ref[...]).T.astype(BF16)
    vg[...] = mm(xgv, wv_ref[...]).astype(BF16)
    for r in range(sp):
        for h in range(heads):
            qg[r, h * share : (h + 1) * share, :] = qgv[r * share : (r + 1) * share, h * head : (h + 1) * head]

    cols = heads * share

    def partial(c, carry):
        s = mm_tb(kloc[...], qg[pl.ds(2 * c, 2)].reshape(2 * cols, head))
        top = jnp.max(s, axis=0, keepdims=True)
        e = jnp.exp(s - top)
        total = jnp.sum(e, axis=0, keepdims=True)
        num = mm(vt[...], e.astype(BF16))
        stats = jnp.concatenate([top, total, jnp.zeros((6, 2 * cols), F32)], axis=0)
        for r in range(2):
            part[c // (chips // 2), lax.rem(c, chips // 2) * 2 + r, 0:head, :] = num[:, r * cols : (r + 1) * cols]
            part[c // (chips // 2), lax.rem(c, chips // 2) * 2 + r, head:, :] = stats[:, r * cols : (r + 1) * cols]
        return carry

    lax.fori_loop(0, sp // 2, partial, 0)
    part_send = [send(part.at[1 - core], pq, part_s.at[0], part_r.at[0], partner)]

    def merge(blocks):
        best = functools.reduce(jnp.maximum, [b[1] for b in blocks])
        num, total = 0.0, 0.0
        for n, t, l in blocks:
            f = jnp.exp(t - best)
            num = num + n * f
            total = total + l * f
        return num, best, total

    def read(ref, i):
        return ref[i, 0:head, :], ref[i, head : head + 1, :], ref[i, head + 1 : head + 2, :]

    for copy in halo:
        copy.wait_recv()
    arrival(pq, part_s.at[0], part_r.at[0], partner).wait_recv()
    for c in range(chips):
        mine_c = part[core, c]
        num, best, total = merge([
            (mine_c[0:head], mine_c[head : head + 1], mine_c[head + 1 : head + 2]), read(pq, c)])
        pc[c, 0:head, :] = num
        pc[c, head:, :] = jnp.concatenate([best, total, jnp.zeros((6, cols), F32)], axis=0)
    for k in range(1, chips):
        there = lax.rem(chip + k, chips)
        part_send.append(send(pc.at[there], pr.at[k - 1], part_s.at[k], part_r.at[k], there * 2 + core))

    def window(b, carry):
        off = pl.multiple_of(b * QB, QB)
        q = qs[b]
        s = mm(q, kt[:, pl.ds(off, span)]) + tile[...] + kmask[:, pl.ds(off, span)]
        sg = mm(q, ktg[...])
        top = jnp.maximum(jnp.max(s, axis=1, keepdims=True), jnp.max(sg, axis=1, keepdims=True))
        e = jnp.exp(s - top)
        eg = jnp.exp(sg - top)
        total = jnp.sum(e, axis=1, keepdims=True) + jnp.sum(eg, axis=1, keepdims=True)
        o = mm(e.astype(BF16), vext[pl.ds(off, span), :]) + mm(eg.astype(BF16), vg[...])
        o = (o / total).astype(BF16)
        for h in range(heads):
            att[pl.ds(off, QB), h * head : (h + 1) * head] = o[h * QB : (h + 1) * QB]
        return carry

    lax.fori_loop(0, rows // QB, window, 0)

    loads[4].wait()

    def finish(b, carry):
        off = pl.multiple_of(b * 2 * QB, 2 * QB)
        o = mm(att[pl.ds(off, 2 * QB), :], wo_ref[...])
        h_ref[pl.ds(off, 2 * QB), :] = (x_ref[pl.ds(off, 2 * QB), :].astype(F32) + o).astype(BF16)
        return carry

    lax.fori_loop(0, rows // (2 * QB), finish, 0)

    for k in range(1, chips):
        arrival(pr.at[k - 1], part_s.at[k], part_r.at[k], partner).wait_recv()
    num, best, total = merge([read(pc, chip)] + [read(pr, k - 1) for k in range(1, chips)])
    og = (num / total).T.astype(BF16)
    ag = jnp.concatenate([og[h * share : (h + 1) * share] for h in range(heads)], axis=1)
    hg = xg[core * chips + chip].astype(F32) + mm(ag, wo_ref[...])
    h_ref[rows : rows + share, :] = hg.astype(BF16)
    for copy in halo + part_send:
        copy.wait_send()


def attention(sp, x, wq, wk, wv, wo, rel, gp, heads):
    rows, dim = x.shape
    head = wk.shape[1]
    width = (rel.shape[1] - 1) // 2
    span, ext = 2 * width + QB, rows + 2 * width
    n_glob = gp.shape[1]
    share, chips = n_glob // sp, sp // 2
    cols = heads * share
    anyspec = pl.BlockSpec(memory_space=pl.ANY)
    vmem = pl.BlockSpec(memory_space=pltpu.VMEM)
    dma = pltpu.SemaphoreType.DMA
    V = pltpu.VMEM
    return pl.pallas_call(
        functools.partial(attention_kernel, sp, heads),
        out_shape=jax.ShapeDtypeStruct((rows + share, dim), BF16),
        in_specs=[anyspec] * 5 + [vmem] * 2,
        out_specs=vmem,
        scratch_shapes=[
            V(x.shape, BF16), V(wq.shape, BF16), V(wk.shape, BF16), V(wv.shape, BF16), V(wo.shape, BF16),
            V((heads, span), F32), V((heads * QB, span), F32), V((ext, n_glob), BF16), V((1, ext), F32),
            V((head, ext), BF16), V((rows, head), BF16), V((head, rows), BF16), V((ext, head), BF16),
            V((rows // QB, heads * QB, head), BF16), V((sp, cols, head), BF16),
            V((head, n_glob), BF16), V((n_glob, head), BF16), V((rows, heads * head), BF16),
            V((2, chips, share, dim), BF16), V((chips, share, dim), BF16), V((chips, share, dim), BF16),
            V((chips - 1, share, dim), BF16), V((sp, share, dim), BF16),
            V((2, chips, head + 8, cols), F32), V((chips, head + 8, cols), F32),
            V((chips, head + 8, cols), F32), V((chips - 1, head + 8, cols), F32),
            dma((5,)), dma((4,)), dma((4,)), dma((chips,)), dma((chips,)), dma((chips,)), dma((chips,)),
            dma((chips,)), dma((chips,)),
        ],
        compiler_params=pltpu.CompilerParams(
            collective_id=0, has_side_effects=True, vmem_limit_bytes=VMEM_LIMIT),
        name='attend',
    )(x, wq, wk, wv, wo, rel, gp)


def ffn_kernel(sp, chunk, parts, h_ref, wu_hbm, wd_hbm, y_ref, yg_ref, wu, wd, acc, ubuf, gbuf, wu_sem, wd_sem, ssem, rsem):
    me = lax.axis_index('sp')
    chips = sp // 2
    chip, core = me // 2, lax.rem(me, 2)
    n_chunks = wu.shape[0]
    total = h_ref.shape[0]
    rows = y_ref.shape[0]
    share = total - rows
    tile = total // parts

    def up_copy(c):
        return pltpu.make_async_copy(wu_hbm.at[:, pl.ds(pl.multiple_of(c * chunk, chunk), chunk)], wu.at[c], wu_sem.at[c])

    def down_copy(c):
        return pltpu.make_async_copy(wd_hbm.at[pl.ds(pl.multiple_of(c * chunk, chunk), chunk), :], wd.at[c], wd_sem.at[c])

    def begin(c, carry):
        up_copy(c).start()
        down_copy(c).start()
        return carry

    lax.fori_loop(0, n_chunks, begin, 0)
    barrier = greet(sp)
    sends = []
    for p in range(parts):
        off = (parts - 1 - p) * tile
        hv = h_ref[off : off + tile, :]
        acc[...] = hv.astype(F32)

        def step(c, carry, p=p, off=off):
            if p == 0:
                up_copy(c).wait()
                down_copy(c).wait()
            z = mm(h_ref[off : off + tile, :], wu[c])
            u = jax.nn.gelu(z).astype(BF16)
            acc[...] += mm(u, wd[c])
            return carry

        lax.fori_loop(0, n_chunks, step, 0)
        y = acc[...].astype(BF16)
        if p == 0:
            y_ref[off:rows, :] = y[: tile - share]
            gbuf[core * chips + chip] = y[tile - share :]
            pl.semaphore_wait(barrier, sp - 1)
            sends = gather_blocks(gbuf, chips, chip, core, ssem, rsem)
        else:
            y_ref[off : off + tile, :] = y
        if p == 1:
            sends.append(gather_forward(gbuf, chips, chip, core, ssem, rsem))
    gather_finish(gbuf, chips, chip, core, ssem, rsem, sends)
    yg_ref[...] = gbuf[...].reshape(yg_ref.shape)


def ffn(sp, h, wu, wd, rows, chunk=384, parts=3):
    total, dim = h.shape
    hidden = wu.shape[1]
    share = total - rows
    n_chunks = hidden // chunk
    chips = sp // 2
    anyspec = pl.BlockSpec(memory_space=pl.ANY)
    vmem = pl.BlockSpec(memory_space=pltpu.VMEM)
    dma = pltpu.SemaphoreType.DMA
    V = pltpu.VMEM
    return pl.pallas_call(
        functools.partial(ffn_kernel, sp, chunk, parts),
        out_shape=(jax.ShapeDtypeStruct((rows, dim), BF16), jax.ShapeDtypeStruct((share * sp, dim), BF16)),
        in_specs=[vmem, anyspec, anyspec],
        out_specs=(vmem, vmem),
        scratch_shapes=[
            V((n_chunks, dim, chunk), BF16), V((n_chunks, chunk, dim), BF16), V((total // parts, dim), F32),
            V((total // parts, chunk), BF16), V((sp, share, dim), BF16),
            dma((n_chunks,)), dma((n_chunks,)), dma((chips,)), dma((chips,)),
        ],
        compiler_params=pltpu.CompilerParams(
            collective_id=1, has_side_effects=True, vmem_limit_bytes=VMEM_LIMIT),
        name='feed',
    )(h, wu, wd)


def solution(mesh):
    sp = mesh.shape['sp']

    def shard_layer(hidden_in, w_query, w_key, w_value, w_out, w_up, w_down, rel_bias, glob_pos):
        rows, dim = hidden_in.shape
        heads, head = w_query.shape[1], w_query.shape[2]
        h = attention(
            sp, hidden_in, w_query.reshape(dim, heads * head), w_key.reshape(dim, head), w_value.reshape(dim, head),
            w_out.reshape(heads * head, dim), rel_bias, glob_pos[None, :], heads)
        y, y_glob = ffn(sp, h, w_up, w_down, rows)
        pos = lax.axis_index('sp') * rows + jnp.arange(rows)
        hit = pos[:, None] == glob_pos[None, :]
        placed = jnp.dot(hit.astype(BF16), y_glob, preferred_element_type=F32).astype(BF16)
        y_out = jnp.where(jnp.any(hit, axis=1)[:, None], placed, y)
        return y_out, y_glob

    return jax.shard_map(
        shard_layer, mesh=mesh,
        in_specs=(P(('dp', 'sp'), None), P(), P(), P(), P(), P(), P(), P(), P('dp')),
        out_specs=(P(('dp', 'sp'), None), P('dp', None)),
        check_vma=False)
```

```python
import functools

import jax
import jax.numpy as jnp
from jax import lax
from jax.experimental import pallas as pl
from jax.experimental.pallas import tpu as pltpu
from jax.sharding import PartitionSpec as P

MESH = pl.DeviceIdType.MESH
F32 = jnp.float32
BF16 = jnp.bfloat16
QB = 128
VMEM_LIMIT = 60 * 1024 * 1024


def mm(a, b):
    return jnp.dot(a, b, preferred_element_type=F32)


def mm_ta(a, b):
    return lax.dot_general(a, b, (((0,), (0,)), ((), ())), preferred_element_type=F32)


def mm_tb(a, b):
    return lax.dot_general(a, b, (((1,), (1,)), ((), ())), preferred_element_type=F32)


def send(src, dst, ssem, rsem, dev):
    copy = pltpu.make_async_remote_copy(
        src_ref=src, dst_ref=dst, send_sem=ssem, recv_sem=rsem, device_id={'sp': dev}, device_id_type=MESH)
    copy.start()
    return copy


def arrival(ref, ssem, rsem, dev):
    return pltpu.make_async_remote_copy(
        src_ref=ref, dst_ref=ref, send_sem=ssem, recv_sem=rsem, device_id={'sp': dev}, device_id_type=MESH)


def greet(sp):
    me = lax.axis_index('sp')
    barrier = pltpu.get_barrier_semaphore()
    for k in range(1, sp):
        pl.semaphore_signal(barrier, inc=1, device_id={'sp': lax.rem(me + k, sp)}, device_id_type=MESH)
    return barrier


class Place:
    def __init__(self, sp):
        me = lax.axis_index('sp')
        chips = sp // 2
        assert chips == 4
        self.me, self.chips = me, chips
        self.chip, self.core = me // 2, lax.rem(me, 2)
        self.nxt = lax.rem(self.chip + 1 - 2 * self.core + chips, chips)
        self.prv = lax.rem(self.chip - 1 + 2 * self.core + chips, chips)
        self.far = lax.rem(self.chip + 2, chips)
        self.to_nxt, self.to_prv = self.nxt * 2 + self.core, self.prv * 2 + self.core
        self.partner = self.chip * 2 + 1 - self.core
        self.base, self.other = self.core * chips, (1 - self.core) * chips


class Gather:
    def __init__(self, at, buf, ss, rs):
        self.at, self.buf, self.ss, self.rs = at, buf, ss, rs

    def push(self, chip, k, dev):
        ref = self.buf.at[self.at.base + chip]
        send(ref, ref, self.ss.at[k], self.rs.at[k], dev)

    def landed(self, slot, k):
        arrival(self.buf.at[slot], self.ss.at[k], self.rs.at[k], self.at.partner).wait_recv()

    def start(self):
        at = self.at
        self.push(at.chip, 0, at.to_nxt)
        self.push(at.chip, 1, at.to_prv)
        self.push(at.chip, 3, at.partner)

    def hop(self):
        at = self.at
        self.landed(at.base + at.prv, 0)
        self.push(at.prv, 2, at.to_nxt)
        self.push(at.prv, 4, at.partner)

    def end(self):
        at = self.at
        self.landed(at.base + at.nxt, 1)
        self.push(at.nxt, 5, at.partner)
        self.landed(at.base + at.far, 2)
        self.push(at.far, 6, at.partner)

    def finish(self):
        at = self.at
        for k, chip in ((3, at.chip), (4, at.nxt), (5, at.prv), (6, at.far)):
            self.landed(at.other + chip, k)
        for k, chip in ((0, at.chip), (1, at.chip), (2, at.prv), (3, at.chip), (4, at.prv), (5, at.nxt), (6, at.far)):
            arrival(self.buf.at[at.base + chip], self.ss.at[k], self.rs.at[k], at.partner).wait_send()


def merge(head, blocks):
    best = functools.reduce(jnp.maximum, [v[head : head + 1] for v in blocks])
    num, total = 0.0, 0.0
    for v in blocks:
        f = jnp.exp(v[head : head + 1] - best)
        num = num + v[0:head] * f
        total = total + v[head + 1 : head + 2] * f
    return num, best, total


def pack(ref, slot, head, num, best, total):
    ref[slot, 0:head, :] = num
    ref[slot, head:, :] = jnp.concatenate([best, total, jnp.zeros((6, best.shape[1]), F32)], axis=0)


def attention_kernel(sp, x_hbm, wq_hbm, wk_hbm, wv_hbm, wo_hbm, rel_ref, gp_ref, h_hbm, part_hbm, mine_hbm,
                     x_ref, wq3, wq_ref, wk_ref, wv_ref, wo_ref, rel_pad, tile, onehot, kmask,
                     kt, kloc, vt, vext, qs, qg, ktg, vg, num_ref, top_ref, sum_ref, att, h_ref,
                     xp, xq, xs, xr, xg, part, pq,
                     load_sem, out_sem, halo_s, halo_r, pick_s, pick_r, xg_s, xg_r, part_s, part_r):
    at = Place(sp)
    me, chips = at.me, at.chips
    rows, dim = x_ref.shape
    heads, head = wq3.shape[1:]
    width = (rel_ref.shape[1] - 1) // 2
    span = 2 * width + QB
    n_glob = gp_ref.shape[1]
    share = n_glob // sp
    cols = heads * share
    ext = rows + 2 * width
    seq = rows * sp
    start = me * rows
    blocks = rows // QB
    scale = head ** -0.5

    loads = []
    for i, (src, dst) in enumerate(((x_hbm, x_ref), (wk_hbm, wk_ref), (wv_hbm, wv_ref), (wq_hbm, wq3), (wo_hbm, wo_ref))):
        copy = pltpu.make_async_copy(src, dst, load_sem.at[i])
        copy.start()
        loads.append(copy)
    barrier = greet(sp)

    pos = start - width + lax.broadcasted_iota(jnp.int32, (ext, n_glob), 0)
    onehot[...] = jnp.where(pos == gp_ref[...], 1.0, 0.0).astype(BF16)

    loads[0].wait()
    picked = mm_ta(onehot[width : width + rows, :], x_ref[...]).astype(BF16)
    xp[...] = picked.reshape(xp.shape)
    pl.semaphore_wait(barrier, sp - 1)
    pick_send = [send(xp.at[1 - at.core], xq, pick_s.at[0], pick_r.at[0], at.partner)]

    loads[1].wait()
    k32 = mm(x_ref[...], wk_ref[...])
    kloc[...] = k32.astype(BF16)
    kt[:, width : width + rows] = k32.T.astype(BF16)

    arrival(xq, pick_s.at[0], pick_r.at[0], at.partner).wait_recv()
    xs[...] = xp[at.core] + xq[...]
    pick_send.append(send(xs.at[at.far], xr.at[2], pick_s.at[2], pick_r.at[2], at.to_nxt))
    pick_send.append(send(xs.at[at.prv], xr.at[1], pick_s.at[1], pick_r.at[1], at.to_prv))

    loads[2].wait()
    v32 = mm(x_ref[...], wv_ref[...])
    vext[width : width + rows, :] = v32.astype(BF16)
    vt[...] = v32.T.astype(BF16)
    right, left = lax.rem(me + 1, sp), lax.rem(me + sp - 1, sp)
    halo = [
        send(kt.at[:, pl.ds(rows, width)], kt.at[:, pl.ds(0, width)], halo_s.at[0], halo_r.at[0], right),
        send(kt.at[:, pl.ds(width, width)], kt.at[:, pl.ds(width + rows, width)], halo_s.at[1], halo_r.at[1], left),
        send(vext.at[pl.ds(rows, width)], vext.at[pl.ds(0, width)], halo_s.at[2], halo_r.at[2], right),
        send(vext.at[pl.ds(width, width)], vext.at[pl.ds(width + rows, width)], halo_s.at[3], halo_r.at[3], left),
    ]

    count = mm_tb(jnp.ones((8, n_glob), BF16), onehot[...])[0:1]
    col = start - width + lax.broadcasted_iota(jnp.int32, (1, ext), 1)
    kmask[...] = jnp.where((count > 0.5) | (col < 0) | (col >= seq), -jnp.inf, 0.0)
    rel_pad[...] = jnp.full(rel_pad.shape, -jnp.inf, F32)
    rel_pad[:, : 2 * width + 1] = rel_ref[...]
    for h in range(heads):
        line = jnp.broadcast_to(rel_pad[h : h + 1, :], (QB, span))
        tile[h * QB : (h + 1) * QB, :] = pltpu.roll(line, 0, 1, stride=1, stride_axis=0)

    loads[3].wait()
    wq_ref[...] = wq3[...].reshape(wq_ref.shape)

    arrival(xr.at[2], pick_s.at[2], pick_r.at[2], at.partner).wait_recv()
    xs[at.nxt] = xs[at.nxt] + xr[2]
    pick_send.append(send(xs.at[at.nxt], xr.at[0], pick_s.at[3], pick_r.at[3], at.to_nxt))

    for b in range(0, blocks, 2):
        qb = (mm(x_ref[b * QB : (b + 2) * QB, :], wq_ref[...]) * scale).astype(BF16)
        for r in range(2):
            for h in range(heads):
                qs[b + r, h * QB : (h + 1) * QB, :] = qb[r * QB : (r + 1) * QB, h * head : (h + 1) * head]

    arrival(xr.at[0], pick_s.at[3], pick_r.at[3], at.partner).wait_recv()
    arrival(xr.at[1], pick_s.at[1], pick_r.at[1], at.partner).wait_recv()
    xg[at.base + at.chip] = xs[at.chip] + xr[0] + xr[1]
    gather = Gather(at, xg, xg_s, xg_r)
    gather.start()
    outs = [pltpu.make_async_copy(xg.at[at.base + at.chip], mine_hbm, out_sem.at[0])]
    outs[0].start()

    def window(b):
        lo, hi = max(b * QB, width), min(b * QB + span, width + rows)
        s = mm(qs[b], kt[:, lo:hi]) + tile[:, lo - b * QB : hi - b * QB] + kmask[:, lo:hi]
        top = jnp.max(s, axis=1, keepdims=True)
        e = jnp.exp(s - top)
        total = jnp.sum(e, axis=1, keepdims=True)
        num_ref[b] = mm(e.astype(BF16), vext[lo:hi, :])
        top_ref[b] = jnp.broadcast_to(top, top_ref.shape[1:])
        sum_ref[b] = jnp.broadcast_to(total, sum_ref.shape[1:])

    for b in range(blocks // 2):
        window(b)
    gather.hop()
    for b in range(blocks // 2, blocks):
        window(b)
    gather.end()
    gather.finish()

    xgv = xg[...].reshape(n_glob, dim)
    ktg[...] = mm(xgv, wk_ref[...]).T.astype(BF16)
    vg[...] = mm(xgv, wv_ref[...]).astype(BF16)
    qgv = (mm(xgv, wq_ref[...]) * scale).astype(BF16)
    for r in range(sp):
        for h in range(heads):
            qg[r, h * share : (h + 1) * share, :] = qgv[r * share : (r + 1) * share, h * head : (h + 1) * head]

    for c in range(sp // 2):
        s = mm_tb(kloc[...], qg[2 * c : 2 * c + 2].reshape(2 * cols, head))
        top = jnp.max(s, axis=0, keepdims=True)
        e = jnp.exp(s - top)
        total = jnp.sum(e, axis=0, keepdims=True)
        num = mm(vt[...], e.astype(BF16))
        for r in range(2):
            here = slice(r * cols, (r + 1) * cols)
            pack(part, 2 * c + r, head, num[:, here], top[:, here], total[:, here])
    part_send = send(part.at[pl.ds(at.other, chips)], pq, part_s.at[0], part_r.at[0], at.partner)

    for copy in halo:
        copy.wait_recv()

    def complete(b):
        lo, hi = (b * QB, width) if b * QB < width else (width + rows, b * QB + span)
        s = mm(qs[b], kt[:, lo:hi]) + tile[:, lo - b * QB : hi - b * QB] + kmask[:, lo:hi]
        sg = mm(qs[b], ktg[...])
        top = top_ref[b]
        best = jnp.maximum(jnp.max(s, axis=1, keepdims=True), jnp.max(sg, axis=1, keepdims=True))
        best = jnp.maximum(top, best)
        fade = jnp.exp(top - best)
        e = [jnp.exp(s[:, i : i + QB] - best) for i in range(0, hi - lo, QB)]
        eg = [jnp.exp(sg[:, i : i + QB] - best) for i in range(0, n_glob, QB)]
        total = sum_ref[b] * fade + jnp.sum(functools.reduce(jnp.add, e + eg), axis=1, keepdims=True)
        o = mm(jnp.concatenate(e, axis=1).astype(BF16), vext[lo:hi, :])
        o = o + mm(jnp.concatenate(eg, axis=1).astype(BF16), vg[...])
        inv = 1.0 / total
        o = jnp.concatenate(
            [((num_ref[b, :, i : i + QB] * fade + o[:, i : i + QB]) * inv).astype(BF16) for i in range(0, head, QB)], axis=1)
        for h in range(heads):
            att[b * QB : (b + 1) * QB, h * head : (h + 1) * head] = o[h * QB : (h + 1) * QB]

    for b in range(blocks):
        complete(b)

    arrival(pq, part_s.at[0], part_r.at[0], at.partner).wait_recv()
    for c in range(chips):
        pack(pq, c, head, *merge(head, [part[at.base + c], pq[c]]))
    outs.append(pltpu.make_async_copy(pq, part_hbm, out_sem.at[1]))
    outs[-1].start()

    loads[4].wait()
    for b in range(0, blocks, 2):
        here = pl.ds(b * QB, 2 * QB)
        h_ref[here, :] = (x_ref[here, :].astype(F32) + mm(att[here, :], wo_ref[...])).astype(BF16)
        outs.append(pltpu.make_async_copy(h_ref.at[here], h_hbm.at[here], out_sem.at[2 + b // 2]))
        outs[-1].start()
    for copy in halo + pick_send + [part_send]:
        copy.wait_send()
    for copy in outs:
        copy.wait()


def attention(sp, x, wq, wk, wv, wo, rel, gp):
    rows, dim = x.shape
    heads, head = wq.shape[1:]
    width = (rel.shape[1] - 1) // 2
    span, ext = 2 * width + QB, rows + 2 * width
    n_glob = gp.shape[1]
    share, chips = n_glob // sp, sp // 2
    cols = heads * share
    blocks = rows // QB
    anyspec = pl.BlockSpec(memory_space=pl.ANY)
    vmem = pl.BlockSpec(memory_space=pltpu.VMEM)
    dma = pltpu.SemaphoreType.DMA
    V = pltpu.VMEM
    return pl.pallas_call(
        functools.partial(attention_kernel, sp),
        out_shape=(
            jax.ShapeDtypeStruct((rows, dim), BF16),
            jax.ShapeDtypeStruct((chips, head + 8, cols), F32),
            jax.ShapeDtypeStruct((share, dim), BF16)),
        in_specs=[anyspec] * 5 + [vmem] * 2,
        out_specs=(anyspec,) * 3,
        scratch_shapes=[
            V(x.shape, BF16), V(wq.shape, BF16), V((dim, heads * head), BF16), V(wk.shape, BF16), V(wv.shape, BF16), V(wo.shape, BF16),
            V((heads, span), F32), V((heads * QB, span), F32), V((ext, n_glob), BF16), V((1, ext), F32),
            V((head, ext), BF16), V((rows, head), BF16), V((head, rows), BF16), V((ext, head), BF16),
            V((blocks, heads * QB, head), BF16), V((sp, cols, head), BF16),
            V((head, n_glob), BF16), V((n_glob, head), BF16),
            V((blocks, heads * QB, head), F32), V((blocks, heads * QB, QB), F32), V((blocks, heads * QB, QB), F32),
            V((rows, heads * head), BF16), V((rows, dim), BF16),
            V((2, chips, share, dim), BF16), V((chips, share, dim), BF16), V((chips, share, dim), BF16),
            V((chips - 1, share, dim), BF16), V((sp, share, dim), BF16),
            V((sp, head + 8, cols), F32), V((chips, head + 8, cols), F32),
            dma((5,)), dma((2 + blocks // 2,)), dma((4,)), dma((4,)), dma((4,)), dma((4,)), dma((7,)), dma((7,)), dma((1,)), dma((1,)),
        ],
        compiler_params=pltpu.CompilerParams(
            collective_id=0, has_side_effects=True, vmem_limit_bytes=VMEM_LIMIT),
        name='attend',
    )(x, wq, wk, wv, wo, rel, gp)


def gelu(z):
    c = (2.0 / jnp.pi) ** 0.5
    hz = 0.5 * z
    return (hz + hz * jnp.tanh(z * (c + (c * 0.044715) * (z * z)))).astype(BF16)


def ffn_kernel(sp, chunk, group, small, h_hbm, part_hbm, mine_hbm, wo_hbm, wu_hbm, wd_hbm, y_hbm, yg_ref,
               hb, ybuf, wo_ref, wu, wd, acc, ubuf, gbuf, mine_ref, pc, pr,
               in_sem, out_sem, wu_sem, wd_sem, part_s, part_r, ssem, rsem):
    at = Place(sp)
    n_chunks = wu.shape[0]
    rows = ybuf.shape[0]
    share = mine_ref.shape[0]
    cols = pc.shape[2]
    head = pc.shape[1] - 8
    heads = cols // share
    first = rows + share - 2 * small
    cut = first + small - share

    def up(c):
        return pltpu.make_async_copy(wu_hbm.at[:, pl.ds(pl.multiple_of(c * chunk, chunk), chunk)], wu.at[c], wu_sem.at[c])

    def down(c):
        return pltpu.make_async_copy(wd_hbm.at[pl.ds(pl.multiple_of(c * chunk, chunk), chunk), :], wd.at[c], wd_sem.at[c])

    ins = [
        pltpu.make_async_copy(part_hbm, pc, in_sem.at[0]),
        pltpu.make_async_copy(h_hbm.at[pl.ds(0, first)], hb.at[pl.ds(0, first)], in_sem.at[1]),
        pltpu.make_async_copy(mine_hbm, mine_ref, in_sem.at[2]),
        pltpu.make_async_copy(h_hbm.at[pl.ds(first, cut - first)], hb.at[pl.ds(first, cut - first)], in_sem.at[3]),
        pltpu.make_async_copy(h_hbm.at[pl.ds(cut, rows - cut)], hb.at[pl.ds(cut + share, rows - cut)], in_sem.at[4]),
        pltpu.make_async_copy(wo_hbm, wo_ref, in_sem.at[5]),
    ]
    for copy in ins[:2]:
        copy.start()
    for c in range(n_chunks):
        up(c).start()
        down(c).start()
        if c == 2:
            for copy in ins[2:]:
                copy.start()
    barrier = greet(sp)

    def chunks(rows_of, c, n):
        m = rows_of.size
        for j in range(n):
            ubuf[j % 2, 0:m, :] = gelu(mm(hb[rows_of, :], wu[c + j]))
            if j:
                acc[0:m, :] += mm(ubuf[(j - 1) % 2, 0:m, :], wd[c + j - 1])
        acc[0:m, :] += mm(ubuf[(n - 1) % 2, 0:m, :], wd[c + n - 1])

    ins[0].wait()
    pl.semaphore_wait(barrier, sp - 1)
    send(pc.at[at.far], pr.at[2], part_s.at[2], part_r.at[2], at.to_nxt)
    send(pc.at[at.prv], pr.at[1], part_s.at[1], part_r.at[1], at.to_prv)

    ins[1].wait()
    tile0 = pl.ds(0, first)
    acc[0:first, :] = hb[tile0, :].astype(F32)

    def initial(g, carry):
        @pl.when(g == 1)
        def _():
            arrival(pr.at[2], part_s.at[2], part_r.at[2], at.partner).wait_recv()
            pack(pc, at.nxt, head, *merge(head, [pc[at.nxt], pr[2]]))
            send(pc.at[at.nxt], pr.at[0], part_s.at[0], part_r.at[0], at.to_nxt)

        for j in range(group):
            up(g * group + j).wait()
            down(g * group + j).wait()
        chunks(tile0, g * group, group)
        return carry

    lax.fori_loop(0, n_chunks // group, initial, 0)
    ybuf[tile0, :] = acc[0:first, :].astype(BF16)
    outs = [
        pltpu.make_async_copy(ybuf.at[tile0], y_hbm.at[tile0], out_sem.at[0]),
        pltpu.make_async_copy(ybuf.at[pl.ds(first, cut - first)], y_hbm.at[pl.ds(first, cut - first)], out_sem.at[1]),
        pltpu.make_async_copy(ybuf.at[pl.ds(cut, rows - cut)], y_hbm.at[pl.ds(cut, rows - cut)], out_sem.at[2]),
    ]
    outs[0].start()

    for copy in ins[2:]:
        copy.wait()
    for k in range(2):
        arrival(pr.at[k], part_s.at[k], part_r.at[k], at.partner).wait_recv()
    num, best, total = merge(head, [pc[at.chip], pr[0], pr[1]])
    og = (num / total).T.astype(BF16)
    ag = jnp.concatenate([og[h * share : (h + 1) * share] for h in range(heads)], axis=1)
    hb[cut : cut + share, :] = (mine_ref[...].astype(F32) + mm(ag, wo_ref[...])).astype(BF16)

    gather = Gather(at, gbuf, ssem, rsem)

    def later(p, carry):
        here = pl.ds(pl.multiple_of(first + p * small, share), small)
        acc[0:small, :] = hb[here, :].astype(F32)

        def some(g, carry):
            @pl.when((p == 1) & (g == 1))
            def _():
                gather.hop()

            @pl.when((p == 1) & (g == 2))
            def _():
                gather.end()

            chunks(here, g * group, group)
            return carry

        lax.fori_loop(0, n_chunks // group, some, 0)

        @pl.when(p == 0)
        def _():
            ybuf[first:cut, :] = acc[0 : small - share, :].astype(BF16)
            gbuf[at.base + at.chip] = acc[small - share : small, :].astype(BF16)
            gather.start()
            outs[1].start()

        return carry

    lax.fori_loop(0, 2, later, 0)
    ybuf[cut:rows, :] = acc[0:small, :].astype(BF16)
    outs[2].start()
    gather.finish()
    yg_ref[...] = gbuf[...].reshape(yg_ref.shape)
    for k, chip in ((0, at.nxt), (1, at.prv), (2, at.far)):
        arrival(pc.at[chip], part_s.at[k], part_r.at[k], at.partner).wait_send()
    for copy in outs:
        copy.wait()


def ffn(sp, h, part, mine, wo, wu, wd, chunk=768, group=3, small=320):
    rows, dim = h.shape
    share = mine.shape[0]
    n_chunks = wu.shape[1] // chunk
    assert n_chunks == 3 * group
    tile = rows + share - 2 * small
    anyspec = pl.BlockSpec(memory_space=pl.ANY)
    vmem = pl.BlockSpec(memory_space=pltpu.VMEM)
    dma = pltpu.SemaphoreType.DMA
    V = pltpu.VMEM
    return pl.pallas_call(
        functools.partial(ffn_kernel, sp, chunk, group, small),
        out_shape=(jax.ShapeDtypeStruct((rows, dim), BF16), jax.ShapeDtypeStruct((share * sp, dim), BF16)),
        in_specs=[anyspec] * 6,
        out_specs=(anyspec, vmem),
        scratch_shapes=[
            V((rows + share, dim), BF16), V((rows, dim), BF16), V(wo.shape, BF16),
            V((n_chunks, dim, chunk), BF16), V((n_chunks, chunk, dim), BF16), V((tile, dim), F32),
            V((2, tile, chunk), BF16), V((sp, share, dim), BF16),
            V((share, dim), BF16), V(part.shape, F32), V((3,) + part.shape[1:], F32),
            dma((6,)), dma((3,)), dma((n_chunks,)), dma((n_chunks,)), dma((3,)), dma((3,)), dma((7,)), dma((7,)),
        ],
        compiler_params=pltpu.CompilerParams(
            collective_id=1, has_side_effects=True, vmem_limit_bytes=VMEM_LIMIT),
        name='feed',
    )(h, part, mine, wo, wu, wd)


def place_kernel(y_ref, yg_ref, gp_ref, out_ref, outg_ref):
    n, n_glob = y_ref.shape[0], gp_ref.shape[1]
    first = lax.axis_index('sp') * n * pl.num_programs(0) + pl.program_id(0) * n
    pos = first + lax.broadcasted_iota(jnp.int32, (n, n_glob), 0)
    hit = jnp.where(pos == gp_ref[...], 1.0, 0.0)
    here = jnp.sum(hit, axis=1, keepdims=True) > 0.5
    out_ref[...] = jnp.where(here, mm(hit.astype(BF16), yg_ref[...]), y_ref[...].astype(F32)).astype(BF16)
    outg_ref[...] = yg_ref[...]


def place(y, y_glob, gp, steps=2):
    rows, dim = y.shape
    n = rows // steps
    whole = pl.BlockSpec(y_glob.shape, lambda i: (0, 0))
    return pl.pallas_call(
        place_kernel,
        grid=(steps,),
        out_shape=(jax.ShapeDtypeStruct(y.shape, BF16), jax.ShapeDtypeStruct(y_glob.shape, BF16)),
        in_specs=[pl.BlockSpec((n, dim), lambda i: (i, 0)), whole, pl.BlockSpec(gp.shape, lambda i: (0, 0))],
        out_specs=(pl.BlockSpec((n, dim), lambda i: (i, 0)), whole),
        name='place',
    )(y, y_glob, gp)


def solution(mesh):
    sp = mesh.shape['sp']

    def shard_layer(hidden_in, w_query, w_key, w_value, w_out, w_up, w_down, rel_bias, glob_pos):
        dim = hidden_in.shape[1]
        heads, head = w_query.shape[1], w_query.shape[2]
        gp = glob_pos[None, :]
        wo = w_out.reshape(heads * head, dim)
        h, part, mine = attention(
            sp, hidden_in, w_query, w_key.reshape(dim, head), w_value.reshape(dim, head), wo, rel_bias, gp)
        y, y_glob = ffn(sp, h, part, mine, wo, w_up, w_down)
        return place(y, y_glob, gp)

    return jax.shard_map(
        shard_layer, mesh=mesh,
        in_specs=(P(('dp', 'sp'), None), P(), P(), P(), P(), P(), P(), P(), P('dp')),
        out_specs=(P(('dp', 'sp'), None), P('dp', None)),
        check_vma=False)
```

```python
import functools

import jax
import jax.numpy as jnp
from jax import lax
from jax.experimental import pallas as pl
from jax.experimental.pallas import tpu as pltpu
from jax.sharding import PartitionSpec as P

MESH = pl.DeviceIdType.MESH
F32 = jnp.float32
BF16 = jnp.bfloat16
QB = 128
VMEM_LIMIT = 60 * 1024 * 1024


def mm(a, b):
    return jnp.dot(a, b, preferred_element_type=F32)


def mm_ta(a, b):
    return lax.dot_general(a, b, (((0,), (0,)), ((), ())), preferred_element_type=F32)


def mm_tb(a, b):
    return lax.dot_general(a, b, (((1,), (1,)), ((), ())), preferred_element_type=F32)


def send(src, dst, ssem, rsem, dev):
    copy = pltpu.make_async_remote_copy(
        src_ref=src, dst_ref=dst, send_sem=ssem, recv_sem=rsem, device_id={'sp': dev}, device_id_type=MESH)
    copy.start()
    return copy


def arrival(ref, ssem, rsem, dev):
    return pltpu.make_async_remote_copy(
        src_ref=ref, dst_ref=ref, send_sem=ssem, recv_sem=rsem, device_id={'sp': dev}, device_id_type=MESH)


def greet(sp):
    me = lax.axis_index('sp')
    barrier = pltpu.get_barrier_semaphore()
    for k in range(1, sp):
        pl.semaphore_signal(barrier, inc=1, device_id={'sp': lax.rem(me + k, sp)}, device_id_type=MESH)
    return barrier


class Place:
    def __init__(self, sp):
        me = lax.axis_index('sp')
        chips = sp // 2
        assert chips == 4
        self.me, self.chips = me, chips
        self.chip, self.core = me // 2, lax.rem(me, 2)
        self.nxt = lax.rem(self.chip + 1 - 2 * self.core + chips, chips)
        self.prv = lax.rem(self.chip - 1 + 2 * self.core + chips, chips)
        self.far = lax.rem(self.chip + 2, chips)
        self.to_nxt, self.to_prv = self.nxt * 2 + self.core, self.prv * 2 + self.core
        self.partner = self.chip * 2 + 1 - self.core
        self.base, self.other = self.core * chips, (1 - self.core) * chips


class Gather:
    def __init__(self, at, buf, ss, rs):
        self.at, self.buf, self.ss, self.rs = at, buf, ss, rs

    def push(self, chip, k, dev):
        ref = self.buf.at[self.at.base + chip]
        send(ref, ref, self.ss.at[k], self.rs.at[k], dev)

    def landed(self, slot, k):
        arrival(self.buf.at[slot], self.ss.at[k], self.rs.at[k], self.at.partner).wait_recv()

    def start(self):
        at = self.at
        self.push(at.chip, 0, at.to_nxt)
        self.push(at.chip, 1, at.to_prv)
        self.push(at.chip, 3, at.partner)

    def hop(self):
        at = self.at
        self.landed(at.base + at.prv, 0)
        self.push(at.prv, 2, at.to_nxt)
        self.push(at.prv, 4, at.partner)

    def end(self):
        at = self.at
        self.landed(at.base + at.nxt, 1)
        self.push(at.nxt, 5, at.partner)
        self.landed(at.base + at.far, 2)
        self.push(at.far, 6, at.partner)

    def finish(self):
        at = self.at
        for k, chip in ((3, at.chip), (4, at.nxt), (5, at.prv), (6, at.far)):
            self.landed(at.other + chip, k)
        for k, chip in ((0, at.chip), (1, at.chip), (2, at.prv), (3, at.chip), (4, at.prv), (5, at.nxt), (6, at.far)):
            arrival(self.buf.at[at.base + chip], self.ss.at[k], self.rs.at[k], at.partner).wait_send()


def merge(head, blocks):
    best = functools.reduce(jnp.maximum, [v[head : head + 1] for v in blocks])
    num, total = 0.0, 0.0
    for v in blocks:
        f = jnp.exp(v[head : head + 1] - best)
        num = num + v[0:head] * f
        total = total + v[head + 1 : head + 2] * f
    return num, best, total


def pack(ref, slot, head, num, best, total):
    ref[slot, 0:head, :] = num
    ref[slot, head:, :] = jnp.concatenate([best, total, jnp.zeros((6, best.shape[1]), F32)], axis=0)


def layer_kernel(sp, chunk, small, x_hbm, wq_hbm, wk_hbm, wv_hbm, wo_hbm, wu_hbm, wd_hbm, rel_ref, gp_ref, y_hbm, yg_ref,
                 x_ref, wo_ref, kt, vext, xp, xq, xs, xr, xg, part, pc, pr, hb, gbuf, wu_a, wd_a,
                 load_sem, out_sem, wu_sem, wd_sem, halo_s, halo_r, pick_s, pick_r, xg_s, xg_r, part_s, part_r, pass_s, pass_r, yg_s, yg_r):
    at = Place(sp)
    me, chips = at.me, at.chips
    rows, dim = x_ref.shape
    heads, head = wq_hbm.shape[1:]
    width = (rel_ref.shape[1] - 1) // 2
    span = 2 * width + QB
    n_glob = gp_ref.shape[1]
    share = n_glob // sp
    cols = heads * share
    ext = rows + 2 * width
    seq = rows * sp
    start = me * rows
    blocks = rows // QB
    scale = head ** -0.5
    n_chunks = wu_hbm.shape[1] // chunk
    early = wu_a.shape[0]
    first = rows + share - 2 * small
    cut = first + small - share

    def up_to(c, ref):
        return pltpu.make_async_copy(wu_hbm.at[:, pl.ds(pl.multiple_of(c * chunk, chunk), chunk)], ref, wu_sem.at[c])

    def down_to(c, ref):
        return pltpu.make_async_copy(wd_hbm.at[pl.ds(pl.multiple_of(c * chunk, chunk), chunk), :], ref, wd_sem.at[c])

    early_loads = [up_to(c, wu_a.at[c]) for c in range(early)] + [down_to(c, wd_a.at[c]) for c in range(early - 1)]
    right, left = lax.rem(me + 1, sp), lax.rem(me + sp - 1, sp)
    barrier = greet(sp)

    def attend(wq3, wq_ref, wk_ref, wv_ref, rel_pad, tile, onehot, kmask, kloc, vt, qs, qg, ktg, vg, num_ref, top_ref, sum_ref, att):
        loads = []
        for i, (src, dst) in enumerate(((x_hbm, x_ref), (wk_hbm, wk_ref), (wv_hbm, wv_ref), (wq_hbm, wq3), (wo_hbm, wo_ref))):
            loads.append(pltpu.make_async_copy(src, dst, load_sem.at[i]))
        loads[0].start()
        loads[1].start()

        pos = start - width + lax.broadcasted_iota(jnp.int32, (ext, n_glob), 0)
        onehot[...] = jnp.where(pos == gp_ref[...], 1.0, 0.0).astype(BF16)

        count = mm_tb(jnp.ones((8, n_glob), BF16), onehot[...])[0:1]
        col = start - width + lax.broadcasted_iota(jnp.int32, (1, ext), 1)
        kmask[...] = jnp.where((count > 0.5) | (col < 0) | (col >= seq), -jnp.inf, 0.0)
        rel_pad[...] = jnp.full(rel_pad.shape, -jnp.inf, F32)
        rel_pad[:, : 2 * width + 1] = rel_ref[...]
        for h in range(heads):
            line = jnp.broadcast_to(rel_pad[h : h + 1, :], (QB, span))
            tile[h * QB : (h + 1) * QB, :] = pltpu.roll(line, 0, 1, stride=1, stride_axis=0)

        def pick(rank):
            some = pl.ds(pl.multiple_of(rank * share, QB), chips * share)
            return mm_ta(onehot[width : width + rows, some], x_ref[...]).astype(BF16).reshape(xp.shape)

        loads[0].wait()
        for copy in loads[2:]:
            copy.start()
        xp[...] = pick(at.other)
        pl.semaphore_wait(barrier, sp - 1)
        pick_send = [send(xp, xq, pick_s.at[0], pick_r.at[0], at.partner)]
        xs[...] = pick(at.base)

        def key_rows(lo, hi):
            k32 = mm(x_ref[lo:hi, :], wk_ref[...])
            kloc[lo:hi, :] = k32.astype(BF16)
            kt[:, width + lo : width + hi] = k32.T.astype(BF16)

        loads[1].wait()
        key_rows(0, rows // 2)
        arrival(xq, pick_s.at[0], pick_r.at[0], at.partner).wait_recv()
        xs[...] = xs[...] + xq[...]
        pick_send.append(send(xs.at[at.far], xr.at[2], pick_s.at[2], pick_r.at[2], at.to_nxt))
        pick_send.append(send(xs.at[at.prv], xr.at[1], pick_s.at[1], pick_r.at[1], at.to_prv))
        key_rows(rows // 2, rows)

        loads[2].wait()
        v32 = mm(x_ref[...], wv_ref[...])
        vext[width : width + rows, :] = v32.astype(BF16)
        vt[...] = v32.T.astype(BF16)
        halo = [
            send(kt.at[:, pl.ds(rows, width)], kt.at[:, pl.ds(0, width)], halo_s.at[0], halo_r.at[0], right),
            send(kt.at[:, pl.ds(width, width)], kt.at[:, pl.ds(width + rows, width)], halo_s.at[1], halo_r.at[1], left),
            send(vext.at[pl.ds(rows, width)], vext.at[pl.ds(0, width)], halo_s.at[2], halo_r.at[2], right),
            send(vext.at[pl.ds(width, width)], vext.at[pl.ds(width + rows, width)], halo_s.at[3], halo_r.at[3], left),
        ]

        loads[3].wait()
        wq_ref[...] = wq3[...].reshape(wq_ref.shape)

        def project(b):
            qb = (mm(x_ref[b * QB : (b + 2) * QB, :], wq_ref[...]) * scale).astype(BF16)
            for r in range(2):
                for h in range(heads):
                    qs[b + r, h * QB : (h + 1) * QB, :] = qb[r * QB : (r + 1) * QB, h * head : (h + 1) * head]

        project(0)
        arrival(xr.at[2], pick_s.at[2], pick_r.at[2], at.partner).wait_recv()
        xs[at.nxt] = xs[at.nxt] + xr[2]
        pick_send.append(send(xs.at[at.nxt], xr.at[0], pick_s.at[3], pick_r.at[3], at.to_nxt))
        for b in range(2, blocks, 2):
            project(b)

        arrival(xr.at[0], pick_s.at[3], pick_r.at[3], at.partner).wait_recv()
        arrival(xr.at[1], pick_s.at[1], pick_r.at[1], at.partner).wait_recv()
        xg[at.base + at.chip] = xs[at.chip] + xr[0] + xr[1]
        gather = Gather(at, xg, xg_s, xg_r)
        gather.start()
        loads[4].wait()
        for copy in early_loads:
            copy.start()

        def window(b):
            lo = max(b * QB, width)
            hi = b * QB + span if b >= blocks // 2 else min(b * QB + span, width + rows)
            s = mm(qs[b], kt[:, lo:hi]) + tile[:, lo - b * QB : hi - b * QB] + kmask[:, lo:hi]
            top = jnp.max(s, axis=1, keepdims=True)
            e = jnp.exp(s - top)
            total = jnp.sum(e, axis=1, keepdims=True)
            num_ref[b] = mm(e.astype(BF16), vext[lo:hi, :])
            top_ref[b] = jnp.broadcast_to(top, top_ref.shape[1:])
            sum_ref[b] = jnp.broadcast_to(total, sum_ref.shape[1:])

        for b in range(blocks // 2):
            window(b)
        gather.hop()
        for copy in halo:
            copy.wait_recv()
        for b in range(blocks // 2, blocks):
            window(b)
        gather.end()

        def global_rows(rank):
            some = pl.ds(pl.multiple_of(rank * share, QB), chips * share)
            xgv = xg[pl.ds(rank, chips)].reshape(chips * share, dim)
            ktg[:, some] = mm(xgv, wk_ref[...]).T.astype(BF16)
            vg[some, :] = mm(xgv, wv_ref[...]).astype(BF16)
            qgv = (mm(xgv, wq_ref[...]) * scale).astype(BF16)
            for r in range(chips):
                for h in range(heads):
                    qg[r, h * share : (h + 1) * share, :] = qgv[r * share : (r + 1) * share, h * head : (h + 1) * head]
            for c in range(0, chips, 2):
                s = mm_tb(kloc[...], qg[c : c + 2].reshape(2 * cols, head))
                top = jnp.max(s, axis=0, keepdims=True)
                e = jnp.exp(s - top)
                total = jnp.sum(e, axis=0, keepdims=True)
                num = mm(vt[...], e.astype(BF16))
                for r in range(2):
                    here = slice(r * cols, (r + 1) * cols)
                    pack(part, rank + c + r, head, num[:, here], top[:, here], total[:, here])

        def parity(i, carry):
            @pl.when(i == 1)
            def _():
                gather.finish()

            global_rows(lax.rem(at.core + i, 2) * chips)
            return carry

        lax.fori_loop(0, 2, parity, 0)
        part_send = send(part.at[pl.ds(at.other, chips)], pc, part_s.at[0], part_r.at[0], at.partner)

        def complete(b):
            lo, hi = b * QB, max(b * QB, width)
            scores = [(mm(qs[b], ktg[...]), vg[...])]
            if lo < hi:
                s = mm(qs[b], kt[:, lo:hi]) + tile[:, : hi - lo] + kmask[:, lo:hi]
                scores.append((s, vext[lo:hi, :]))
            if b >= blocks // 2:
                scores = scores[:1]
            top = top_ref[b]
            best = top
            for s, _ in scores:
                best = jnp.maximum(best, jnp.max(s, axis=1, keepdims=True))
            fade = jnp.exp(top - best)
            o, sums = 0.0, 0.0
            for s, v in scores:
                e = [jnp.exp(s[:, i : i + QB] - best) for i in range(0, s.shape[1], QB)]
                sums = sums + functools.reduce(jnp.add, e)
                o = o + mm(jnp.concatenate(e, axis=1).astype(BF16), v)
            inv = 1.0 / (sum_ref[b] * fade + jnp.sum(sums, axis=1, keepdims=True))
            o = jnp.concatenate(
                [((num_ref[b, :, i : i + QB] * fade + o[:, i : i + QB]) * inv).astype(BF16) for i in range(0, head, QB)], axis=1)
            for h in range(heads):
                att[b * QB : (b + 1) * QB, h * head : (h + 1) * head] = o[h * QB : (h + 1) * QB]

        for b in range(blocks):
            complete(b)

        arrival(pc, part_s.at[0], part_r.at[0], at.partner).wait_recv()
        for c in range(chips):
            pack(pc, c, head, *merge(head, [part[at.base + c], pc[c]]))
        send(pc.at[at.far], pr.at[2], pass_s.at[2], pass_r.at[2], at.to_nxt)
        send(pc.at[at.prv], pr.at[1], pass_s.at[1], pass_r.at[1], at.to_prv)

        for b in range(0, blocks, 2):
            lo, hi = b * QB, (b + 2) * QB
            v = (x_ref[lo:hi, :].astype(F32) + mm(att[lo:hi, :], wo_ref[...])).astype(BF16)
            mid = min(max(cut, lo), hi)
            if lo < mid:
                hb[lo:mid, :] = v[: mid - lo]
            if mid < hi:
                hb[mid + share : hi + share, :] = v[mid - lo :]
        for copy in halo + pick_send + [part_send]:
            copy.wait_send()

    V = pltpu.VMEM
    pl.run_scoped(
        attend,
        V(wq_hbm.shape, BF16), V((dim, heads * head), BF16), V(wk_hbm.shape, BF16), V(wv_hbm.shape, BF16),
        V((heads, span), F32), V((heads * QB, span), F32), V((ext, n_glob), BF16), V((1, ext), F32),
        V((rows, head), BF16), V((head, rows), BF16), V((blocks, heads * QB, head), BF16), V((chips, cols, head), BF16),
        V((head, n_glob), BF16), V((n_glob, head), BF16),
        V((blocks, heads * QB, head), F32), V((blocks, heads * QB, QB), F32), V((blocks, heads * QB, QB), F32),
        V((rows, heads * head), BF16))

    def feed(wu_b, wd_b, ybuf, acc, ubuf):
        trips = (n_chunks - early) // 2

        def fetch(g):
            for j in range(2):
                up_to(early + 2 * g + j, wu_b.at[2 * g + j]).start()
                down_to(early + 2 * g + j - 1, wd_b.at[2 * g + j]).start()

        def fetched(g):
            for j in range(2):
                up_to(early + 2 * g + j, wu_b.at[2 * g + j]).wait()
                down_to(early + 2 * g + j - 1, wd_b.at[2 * g + j]).wait()

        last = down_to(n_chunks - 1, wd_b.at[2 * trips])
        fetch(0)

        arrival(pr.at[2], pass_s.at[2], pass_r.at[2], at.partner).wait_recv()
        pack(pc, at.nxt, head, *merge(head, [pc[at.nxt], pr[2]]))
        send(pc.at[at.nxt], pr.at[0], pass_s.at[0], pass_r.at[0], at.to_nxt)
        for copy in early_loads:
            copy.wait()

        def open_tile(rows_of):
            m = rows_of.size
            acc[0:m, :] = hb[rows_of, :].astype(F32)
            for c in range(early):
                ubuf[c % 2, 0:m, :] = gelu(mm(hb[rows_of, :], wu_a[c]))
                if c:
                    acc[0:m, :] += mm(ubuf[(c - 1) % 2, 0:m, :], wd_a[c - 1])

        def two_chunks(rows_of, g):
            m = rows_of.size
            for j in range(2):
                ubuf[1 - j, 0:m, :] = gelu(mm(hb[rows_of, :], wu_b[2 * g + j]))
                acc[0:m, :] += mm(ubuf[j, 0:m, :], wd_b[2 * g + j])

        def close_tile(rows_of):
            m = rows_of.size
            return (acc[0:m, :] + mm(ubuf[0, 0:m, :], wd_b[2 * trips])).astype(BF16)

        tile0 = pl.ds(0, first)
        open_tile(tile0)

        def initial(g, carry):
            fetched(g)

            @pl.when(g < trips - 1)
            def _():
                fetch(g + 1)

            @pl.when(g == trips - 1)
            def _():
                last.start()

            two_chunks(tile0, g)
            return carry

        lax.fori_loop(0, trips, initial, 0)
        last.wait()

        for k in range(2):
            arrival(pr.at[k], pass_s.at[k], pass_r.at[k], at.partner).wait_recv()
        num, best, total = merge(head, [pc[at.chip], pr[0], pr[1]])
        og = (num / total).T.astype(BF16)
        ag = jnp.concatenate([og[h * share : (h + 1) * share] for h in range(heads)], axis=1)
        ybuf[tile0, :] = close_tile(tile0)
        hb[cut : cut + share, :] = (xg[at.base + at.chip].astype(F32) + mm(ag, wo_ref[...])).astype(BF16)
        outs = [
            pltpu.make_async_copy(ybuf.at[tile0], y_hbm.at[tile0], out_sem.at[0]),
            pltpu.make_async_copy(ybuf.at[pl.ds(first, cut - first)], y_hbm.at[pl.ds(first, cut - first)], out_sem.at[1]),
            pltpu.make_async_copy(ybuf.at[pl.ds(cut, rows - cut)], y_hbm.at[pl.ds(cut, rows - cut)], out_sem.at[2]),
        ]
        outs[0].start()

        gather = Gather(at, gbuf, yg_s, yg_r)

        def later(p, carry):
            here = pl.ds(pl.multiple_of(first + p * small, share), small)
            open_tile(here)

            def some(g, carry):
                @pl.when((p == 1) & (g == 0))
                def _():
                    gather.hop()

                @pl.when((p == 1) & (g == trips - 1))
                def _():
                    gather.end()

                two_chunks(here, g)
                return carry

            lax.fori_loop(0, trips, some, 0)
            y = close_tile(here)

            @pl.when(p == 0)
            def _():
                ybuf[first:cut, :] = y[0 : small - share]
                gbuf[at.base + at.chip] = y[small - share :]
                gather.start()
                outs[1].start()

            @pl.when(p == 1)
            def _():
                ybuf[cut:rows, :] = y
                outs[2].start()

            return carry

        lax.fori_loop(0, 2, later, 0)
        gather.finish()
        yg_ref[...] = gbuf[...].reshape(yg_ref.shape)
        for k, chip in ((0, at.nxt), (1, at.prv), (2, at.far)):
            arrival(pc.at[chip], pass_s.at[k], pass_r.at[k], at.partner).wait_send()
        for copy in outs:
            copy.wait()

    late = n_chunks - early
    pl.run_scoped(
        feed,
        V((late, dim, chunk), BF16), V((late + 1, chunk, dim), BF16), V((rows, dim), BF16), V((first, dim), F32),
        V((2, first, chunk), BF16))


def layer(sp, x, wq, wk, wv, wo, wu, wd, rel, gp, chunk=768, small=320, early=3):
    rows, dim = x.shape
    heads, head = wq.shape[1:]
    width = (rel.shape[1] - 1) // 2
    ext = rows + 2 * width
    n_glob = gp.shape[1]
    share, chips = n_glob // sp, sp // 2
    cols = heads * share
    n_chunks = wu.shape[1] // chunk
    assert (n_chunks - early) % 2 == 0
    anyspec = pl.BlockSpec(memory_space=pl.ANY)
    vmem = pl.BlockSpec(memory_space=pltpu.VMEM)
    dma = pltpu.SemaphoreType.DMA
    V = pltpu.VMEM
    return pl.pallas_call(
        functools.partial(layer_kernel, sp, chunk, small),
        out_shape=(jax.ShapeDtypeStruct((rows, dim), BF16), jax.ShapeDtypeStruct((n_glob, dim), BF16)),
        in_specs=[anyspec] * 7 + [vmem] * 2,
        out_specs=(anyspec, vmem),
        scratch_shapes=[
            V(x.shape, BF16), V(wo.shape, BF16), V((head, ext), BF16), V((ext, head), BF16),
            V((chips, share, dim), BF16), V((chips, share, dim), BF16), V((chips, share, dim), BF16),
            V((chips - 1, share, dim), BF16), V((sp, share, dim), BF16),
            V((sp, head + 8, cols), F32), V((chips, head + 8, cols), F32), V((3, head + 8, cols), F32),
            V((rows + share, dim), BF16), V((sp, share, dim), BF16),
            V((early, dim, chunk), BF16), V((early - 1, chunk, dim), BF16),
            dma((5,)), dma((3,)), dma((n_chunks,)), dma((n_chunks,)),
            dma((4,)), dma((4,)), dma((4,)), dma((4,)), dma((7,)), dma((7,)), dma((1,)), dma((1,)), dma((3,)), dma((3,)),
            dma((7,)), dma((7,)),
        ],
        compiler_params=pltpu.CompilerParams(
            collective_id=0, has_side_effects=True, vmem_limit_bytes=VMEM_LIMIT),
        name='layer',
    )(x, wq, wk, wv, wo, wu, wd, rel, gp)


def gelu(z):
    c = (2.0 / jnp.pi) ** 0.5
    hz = 0.5 * z
    return (hz + hz * jnp.tanh(z * (c + (c * 0.044715) * (z * z)))).astype(BF16)


def place_kernel(y_ref, yg_ref, gp_ref, out_ref, outg_ref):
    n, n_glob = y_ref.shape[0], gp_ref.shape[1]
    first = lax.axis_index('sp') * n * pl.num_programs(0) + pl.program_id(0) * n
    pos = first + lax.broadcasted_iota(jnp.int32, (n, n_glob), 0)
    hit = jnp.where(pos == gp_ref[...], 1.0, 0.0)
    here = jnp.sum(hit, axis=1, keepdims=True) > 0.5
    out_ref[...] = jnp.where(here, mm(hit.astype(BF16), yg_ref[...]).astype(BF16), y_ref[...])
    outg_ref[...] = yg_ref[...]


def place(y, y_glob, gp, steps=2):
    rows, dim = y.shape
    n = rows // steps
    whole = pl.BlockSpec(y_glob.shape, lambda i: (0, 0))
    return pl.pallas_call(
        place_kernel,
        grid=(steps,),
        out_shape=(jax.ShapeDtypeStruct(y.shape, BF16), jax.ShapeDtypeStruct(y_glob.shape, BF16)),
        in_specs=[pl.BlockSpec((n, dim), lambda i: (i, 0)), whole, pl.BlockSpec(gp.shape, lambda i: (0, 0))],
        out_specs=(pl.BlockSpec((n, dim), lambda i: (i, 0)), whole),
        name='place',
    )(y, y_glob, gp)


def solution(mesh):
    sp = mesh.shape['sp']

    def shard_layer(hidden_in, w_query, w_key, w_value, w_out, w_up, w_down, rel_bias, glob_pos):
        dim = hidden_in.shape[1]
        heads, head = w_query.shape[1], w_query.shape[2]
        gp = glob_pos[None, :]
        wo = w_out.reshape(heads * head, dim)
        y, y_glob = layer(
            sp, hidden_in, w_query, w_key.reshape(dim, head), w_value.reshape(dim, head), wo, w_up, w_down, rel_bias, gp)
        return place(y, y_glob, gp)

    return jax.shard_map(
        shard_layer, mesh=mesh,
        in_specs=(P(('dp', 'sp'), None), P(), P(), P(), P(), P(), P(), P(), P('dp')),
        out_specs=(P(('dp', 'sp'), None), P('dp', None)),
        check_vma=False)
```

```python
import functools

import jax
import jax.numpy as jnp
from jax import lax
from jax.experimental import pallas as pl
from jax.experimental.pallas import tpu as pltpu
from jax.sharding import PartitionSpec as P

MESH = pl.DeviceIdType.MESH
F32 = jnp.float32
BF16 = jnp.bfloat16
QB = 128
VMEM_LIMIT = 60 * 1024 * 1024


def mm(a, b):
    return jnp.dot(a, b, preferred_element_type=F32)


def mm_ta(a, b):
    return lax.dot_general(a, b, (((0,), (0,)), ((), ())), preferred_element_type=F32)


def mm_tb(a, b):
    return lax.dot_general(a, b, (((1,), (1,)), ((), ())), preferred_element_type=F32)


def send(src, dst, ssem, rsem, dev):
    copy = pltpu.make_async_remote_copy(
        src_ref=src, dst_ref=dst, send_sem=ssem, recv_sem=rsem, device_id={'sp': dev}, device_id_type=MESH)
    copy.start()
    return copy


def arrival(ref, ssem, rsem, dev):
    return pltpu.make_async_remote_copy(
        src_ref=ref, dst_ref=ref, send_sem=ssem, recv_sem=rsem, device_id={'sp': dev}, device_id_type=MESH)


def greet(sp):
    me = lax.axis_index('sp')
    barrier = pltpu.get_barrier_semaphore()
    for k in range(1, sp):
        pl.semaphore_signal(barrier, inc=1, device_id={'sp': lax.rem(me + k, sp)}, device_id_type=MESH)
    return barrier


class Place:
    def __init__(self, sp):
        me = lax.axis_index('sp')
        chips = sp // 2
        assert chips == 4
        self.me, self.chips = me, chips
        self.chip, self.core = me // 2, lax.rem(me, 2)
        self.nxt = lax.rem(self.chip + 1 - 2 * self.core + chips, chips)
        self.prv = lax.rem(self.chip - 1 + 2 * self.core + chips, chips)
        self.far = lax.rem(self.chip + 2, chips)
        self.to_nxt, self.to_prv = self.nxt * 2 + self.core, self.prv * 2 + self.core
        self.to_far = self.far * 2 + self.core
        self.partner = self.chip * 2 + 1 - self.core
        self.base, self.other = self.core * chips, (1 - self.core) * chips


class Gather:
    def __init__(self, at, buf, ss, rs):
        self.at, self.buf, self.ss, self.rs = at, buf, ss, rs

    def push(self, chip, k, dev):
        ref = self.buf.at[self.at.base + chip]
        send(ref, ref, self.ss.at[k], self.rs.at[k], dev)

    def landed(self, slot, k):
        arrival(self.buf.at[slot], self.ss.at[k], self.rs.at[k], self.at.partner).wait_recv()

    def start(self):
        at = self.at
        self.push(at.chip, 0, at.to_nxt)
        self.push(at.chip, 2, at.to_far)
        self.push(at.chip, 1, at.to_prv)
        self.push(at.chip, 3, at.partner)

    def hop(self):
        at = self.at
        self.landed(at.base + at.prv, 0)
        self.push(at.prv, 4, at.partner)

    def end(self):
        at = self.at
        self.landed(at.base + at.nxt, 1)
        self.push(at.nxt, 5, at.partner)
        self.landed(at.base + at.far, 2)
        self.push(at.far, 6, at.partner)

    def finish(self):
        at = self.at
        for k, chip in ((3, at.chip), (4, at.nxt), (5, at.prv), (6, at.far)):
            self.landed(at.other + chip, k)
        for k, chip in ((0, at.chip), (1, at.chip), (2, at.chip), (3, at.chip), (4, at.prv), (5, at.nxt), (6, at.far)):
            arrival(self.buf.at[at.base + chip], self.ss.at[k], self.rs.at[k], at.partner).wait_send()


def merge(head, blocks):
    best = functools.reduce(jnp.maximum, [v[head : head + 1] for v in blocks])
    num, total = 0.0, 0.0
    for v in blocks:
        f = jnp.exp(v[head : head + 1] - best)
        num = num + v[0:head] * f
        total = total + v[head + 1 : head + 2] * f
    return num, best, total


def pack(ref, slot, head, num, best, total):
    ref[slot, 0:head, :] = num
    ref[slot, head:, :] = jnp.concatenate([best, total, jnp.zeros((6, best.shape[1]), F32)], axis=0)


def layer_kernel(sp, chunk, small, x_hbm, wq_hbm, wk_hbm, wv_hbm, wo_hbm, wu_hbm, wd_hbm, rel_ref, gp_ref, y_hbm, yg_hbm,
                 x_ref, wo_ref, kt, vext, xp, xq, xs, xr, xg, part, pc, pr, hb, gbuf, wu_a, wd_a,
                 load_sem, out_sem, wu_sem, wd_sem, halo_s, halo_r, pick_s, pick_r, xg_s, xg_r, part_s, part_r, pass_s, pass_r, yg_s, yg_r):
    at = Place(sp)
    me, chips = at.me, at.chips
    rows, dim = x_ref.shape
    heads, head = wq_hbm.shape[1:]
    width = (rel_ref.shape[1] - 1) // 2
    span = 2 * width + QB
    n_glob = gp_ref.shape[1]
    share = n_glob // sp
    cols = heads * share
    ext = rows + 2 * width
    seq = rows * sp
    start = me * rows
    blocks = rows // QB
    scale = head ** -0.5
    n_chunks = wu_hbm.shape[1] // chunk
    early = wu_a.shape[0]
    cut = 2 * small - share

    def up_to(c, ref):
        return pltpu.make_async_copy(wu_hbm.at[:, pl.ds(pl.multiple_of(c * chunk, chunk), chunk)], ref, wu_sem.at[c])

    def down_to(c, ref):
        return pltpu.make_async_copy(wd_hbm.at[pl.ds(pl.multiple_of(c * chunk, chunk), chunk), :], ref, wd_sem.at[c])

    early_loads = [up_to(c, wu_a.at[c]) for c in range(early)] + [down_to(c, wd_a.at[c]) for c in range(early - 1)]
    right, left = lax.rem(me + 1, sp), lax.rem(me + sp - 1, sp)
    barrier = greet(sp)

    def attend(wq3, wq_ref, wk_ref, wv_ref, rel_pad, tile, onehot, kmask, kloc, vt, qs, qg, ktg, vg, num_ref, top_ref, sum_ref, att):
        loads = []
        for i, (src, dst) in enumerate(((x_hbm, x_ref), (wk_hbm, wk_ref), (wv_hbm, wv_ref), (wq_hbm, wq3), (wo_hbm, wo_ref))):
            loads.append(pltpu.make_async_copy(src, dst, load_sem.at[i]))
        loads[0].start()
        loads[1].start()

        pos = start - width + lax.broadcasted_iota(jnp.int32, (ext, n_glob), 0)
        onehot[...] = jnp.where(pos == gp_ref[...], 1.0, 0.0).astype(BF16)

        count = mm_tb(jnp.ones((8, n_glob), BF16), onehot[...])[0:1]
        col = start - width + lax.broadcasted_iota(jnp.int32, (1, ext), 1)
        kmask[...] = jnp.where((count > 0.5) | (col < 0) | (col >= seq), -jnp.inf, 0.0)
        rel_pad[...] = jnp.full(rel_pad.shape, -jnp.inf, F32)
        rel_pad[:, : 2 * width + 1] = rel_ref[...]
        for h in range(heads):
            line = jnp.broadcast_to(rel_pad[h : h + 1, :], (QB, span))
            tile[h * QB : (h + 1) * QB, :] = pltpu.roll(line, 0, 1, stride=1, stride_axis=0)

        def pick(rank):
            some = pl.ds(pl.multiple_of(rank * share, QB), chips * share)
            return mm_ta(onehot[width : width + rows, some], x_ref[...]).astype(BF16).reshape(xp.shape)

        loads[0].wait()
        for copy in loads[2:]:
            copy.start()
        xp[...] = pick(at.other)
        pl.semaphore_wait(barrier, sp - 1)
        pick_send = [send(xp, xq, pick_s.at[0], pick_r.at[0], at.partner)]
        xs[...] = pick(at.base)

        def key_rows(lo, hi):
            k32 = mm(x_ref[lo:hi, :], wk_ref[...])
            kloc[lo:hi, :] = k32.astype(BF16)
            kt[:, width + lo : width + hi] = k32.T.astype(BF16)

        loads[1].wait()
        key_rows(0, rows // 2)
        arrival(xq, pick_s.at[0], pick_r.at[0], at.partner).wait_recv()
        xs[...] = xs[...] + xq[...]
        pick_send.append(send(xs.at[at.far], xr.at[2], pick_s.at[2], pick_r.at[2], at.to_far))
        pick_send.append(send(xs.at[at.nxt], xr.at[0], pick_s.at[3], pick_r.at[3], at.to_nxt))
        pick_send.append(send(xs.at[at.prv], xr.at[1], pick_s.at[1], pick_r.at[1], at.to_prv))
        key_rows(rows // 2, rows)

        loads[2].wait()
        v32 = mm(x_ref[...], wv_ref[...])
        vext[width : width + rows, :] = v32.astype(BF16)
        vt[...] = v32.T.astype(BF16)
        halo = [
            send(kt.at[:, pl.ds(rows, width)], kt.at[:, pl.ds(0, width)], halo_s.at[0], halo_r.at[0], right),
            send(kt.at[:, pl.ds(width, width)], kt.at[:, pl.ds(width + rows, width)], halo_s.at[1], halo_r.at[1], left),
            send(vext.at[pl.ds(rows, width)], vext.at[pl.ds(0, width)], halo_s.at[2], halo_r.at[2], right),
            send(vext.at[pl.ds(width, width)], vext.at[pl.ds(width + rows, width)], halo_s.at[3], halo_r.at[3], left),
        ]

        loads[3].wait()
        wq_ref[...] = wq3[...].reshape(wq_ref.shape)

        def project(b):
            qb = (mm(x_ref[b * QB : (b + 2) * QB, :], wq_ref[...]) * scale).astype(BF16)
            for r in range(2):
                for h in range(heads):
                    qs[b + r, h * QB : (h + 1) * QB, :] = qb[r * QB : (r + 1) * QB, h * head : (h + 1) * head]

        project(0)
        for b in range(2, blocks, 2):
            project(b)

        arrival(xr.at[0], pick_s.at[3], pick_r.at[3], at.partner).wait_recv()
        arrival(xr.at[1], pick_s.at[1], pick_r.at[1], at.partner).wait_recv()
        arrival(xr.at[2], pick_s.at[2], pick_r.at[2], at.partner).wait_recv()
        xg[at.base + at.chip] = (xs[at.chip] + xr[0]) + (xr[1] + xr[2])
        gather = Gather(at, xg, xg_s, xg_r)
        gather.start()
        loads[4].wait()
        for copy in early_loads:
            copy.start()

        def window(b):
            lo = max(b * QB, width)
            hi = b * QB + span if b >= blocks // 2 else min(b * QB + span, width + rows)
            s = mm(qs[b], kt[:, lo:hi]) + tile[:, lo - b * QB : hi - b * QB] + kmask[:, lo:hi]
            top = jnp.max(s, axis=1, keepdims=True)
            e = jnp.exp(s - top)
            total = jnp.sum(e, axis=1, keepdims=True)
            num_ref[b] = mm(e.astype(BF16), vext[lo:hi, :])
            top_ref[b] = jnp.broadcast_to(top, top_ref.shape[1:])
            sum_ref[b] = jnp.broadcast_to(total, sum_ref.shape[1:])

        for b in range(blocks // 2):
            window(b)
        gather.hop()
        for copy in halo:
            copy.wait_recv()
        for b in range(blocks // 2, blocks):
            window(b)
        gather.end()

        def global_rows(rank):
            some = pl.ds(pl.multiple_of(rank * share, QB), chips * share)
            xgv = xg[pl.ds(rank, chips)].reshape(chips * share, dim)
            ktg[:, some] = mm(xgv, wk_ref[...]).T.astype(BF16)
            vg[some, :] = mm(xgv, wv_ref[...]).astype(BF16)
            qgv = (mm(xgv, wq_ref[...]) * scale).astype(BF16)
            for r in range(chips):
                for h in range(heads):
                    qg[r, h * share : (h + 1) * share, :] = qgv[r * share : (r + 1) * share, h * head : (h + 1) * head]
            for c in range(0, chips, 2):
                s = mm_tb(kloc[...], qg[c : c + 2].reshape(2 * cols, head))
                top = jnp.max(s, axis=0, keepdims=True)
                e = jnp.exp(s - top)
                total = jnp.sum(e, axis=0, keepdims=True)
                num = mm(vt[...], e.astype(BF16))
                for r in range(2):
                    here = slice(r * cols, (r + 1) * cols)
                    pack(part, rank + c + r, head, num[:, here], top[:, here], total[:, here])

        def parity(i, carry):
            @pl.when(i == 1)
            def _():
                gather.finish()

            global_rows(lax.rem(at.core + i, 2) * chips)
            return carry

        lax.fori_loop(0, 2, parity, 0)
        part_send = send(part.at[pl.ds(at.other, chips)], pc, part_s.at[0], part_r.at[0], at.partner)

        def complete(b):
            lo, hi = b * QB, max(b * QB, width)
            scores = [(mm(qs[b], ktg[...]), vg[...])]
            if lo < hi:
                s = mm(qs[b], kt[:, lo:hi]) + tile[:, : hi - lo] + kmask[:, lo:hi]
                scores.append((s, vext[lo:hi, :]))
            if b >= blocks // 2:
                scores = scores[:1]
            top = top_ref[b]
            best = top
            for s, _ in scores:
                best = jnp.maximum(best, jnp.max(s, axis=1, keepdims=True))
            fade = jnp.exp(top - best)
            o, sums = 0.0, 0.0
            for s, v in scores:
                e = [jnp.exp(s[:, i : i + QB] - best) for i in range(0, s.shape[1], QB)]
                sums = sums + functools.reduce(jnp.add, e)
                o = o + mm(jnp.concatenate(e, axis=1).astype(BF16), v)
            inv = 1.0 / (sum_ref[b] * fade + jnp.sum(sums, axis=1, keepdims=True))
            o = jnp.concatenate(
                [((num_ref[b, :, i : i + QB] * fade + o[:, i : i + QB]) * inv).astype(BF16) for i in range(0, head, QB)], axis=1)
            for h in range(heads):
                att[b * QB : (b + 1) * QB, h * head : (h + 1) * head] = o[h * QB : (h + 1) * QB]

        for b in range(blocks):
            complete(b)

        arrival(pc, part_s.at[0], part_r.at[0], at.partner).wait_recv()
        for c in range(chips):
            pack(pc, c, head, *merge(head, [part[at.base + c], pc[c]]))
        send(pc.at[at.far], pr.at[2], pass_s.at[2], pass_r.at[2], at.to_nxt)
        send(pc.at[at.prv], pr.at[1], pass_s.at[1], pass_r.at[1], at.to_prv)

        for b in range(0, blocks, 2):
            lo, hi = b * QB, (b + 2) * QB
            v = (x_ref[lo:hi, :].astype(F32) + mm(att[lo:hi, :], wo_ref[...])).astype(BF16)
            mid = min(max(cut, lo), hi)
            if lo < mid:
                hb[lo:mid, :] = v[: mid - lo]
            if mid < hi:
                hb[mid + share : hi + share, :] = v[mid - lo :]
        for copy in halo + pick_send + [part_send]:
            copy.wait_send()

    V = pltpu.VMEM
    pl.run_scoped(
        attend,
        V(wq_hbm.shape, BF16), V((dim, heads * head), BF16), V(wk_hbm.shape, BF16), V(wv_hbm.shape, BF16),
        V((heads, span), F32), V((heads * QB, span), F32), V((ext, n_glob), BF16), V((1, ext), F32),
        V((rows, head), BF16), V((head, rows), BF16), V((blocks, heads * QB, head), BF16), V((chips, cols, head), BF16),
        V((head, n_glob), BF16), V((n_glob, head), BF16),
        V((blocks, heads * QB, head), F32), V((blocks, heads * QB, QB), F32), V((blocks, heads * QB, QB), F32),
        V((rows, heads * head), BF16))

    def feed(wu_b, wd_b, ybuf, acc, ubuf):
        late_loads = [down_to(early - 1, wd_b.at[0])]
        for c in range(early, n_chunks):
            late_loads += [up_to(c, wu_b.at[c - early]), down_to(c, wd_b.at[c - early + 1])]
        for copy in late_loads:
            copy.start()

        arrival(pr.at[2], pass_s.at[2], pass_r.at[2], at.partner).wait_recv()
        pack(pc, at.nxt, head, *merge(head, [pc[at.nxt], pr[2]]))
        send(pc.at[at.nxt], pr.at[0], pass_s.at[0], pass_r.at[0], at.to_nxt)
        for copy in early_loads:
            copy.wait()

        gather = Gather(at, gbuf, yg_s, yg_r)
        ends = (0, small, 2 * small - share, rows)
        outs = [
            pltpu.make_async_copy(ybuf.at[pl.ds(a, b - a)], y_hbm.at[pl.ds(a, b - a)], out_sem.at[p])
            for p, (a, b) in enumerate(zip(ends[:-1], ends[1:]))]

        def one_tile(p, carry):
            here = pl.ds(pl.multiple_of(p * small, share), small)
            acc[...] = hb[here, :].astype(F32)
            for c in range(early):
                ubuf[c % 2] = gelu(mm(hb[here, :], wu_a[c]))
                if c:
                    acc[...] += mm(ubuf[(c - 1) % 2], wd_a[c - 1])

            @pl.when(p == 0)
            def _():
                for copy in late_loads:
                    copy.wait()
                for k in range(2):
                    arrival(pr.at[k], pass_s.at[k], pass_r.at[k], at.partner).wait_recv()
                num, best, total = merge(head, [pc[at.chip], pr[0], pr[1]])
                og = (num / total).T.astype(BF16)
                ag = jnp.concatenate([og[h * share : (h + 1) * share] for h in range(heads)], axis=1)
                hb[cut : cut + share, :] = (xg[at.base + at.chip].astype(F32) + mm(ag, wo_ref[...])).astype(BF16)

            @pl.when(p == 2)
            def _():
                gather.hop()
                gather.end()

            for c in range(early, n_chunks):
                ubuf[c % 2] = gelu(mm(hb[here, :], wu_b[c - early]))
                acc[...] += mm(ubuf[(c - 1) % 2], wd_b[c - early])
            y = (acc[...] + mm(ubuf[(n_chunks - 1) % 2], wd_b[n_chunks - early])).astype(BF16)

            @pl.when(p == 0)
            def _():
                ybuf[0:small, :] = y
                outs[0].start()

            @pl.when(p == 1)
            def _():
                ybuf[small:cut, :] = y[0 : small - share]
                gbuf[at.base + at.chip] = y[small - share :]
                gather.start()
                outs[1].start()

            @pl.when(p == 2)
            def _():
                ybuf[cut:rows, :] = y
                outs[2].start()

            return carry

        lax.fori_loop(0, 3, one_tile, 0)
        gather.finish()
        outs.append(pltpu.make_async_copy(gbuf, yg_hbm, out_sem.at[3]))
        outs[3].start()
        for k, chip in ((0, at.nxt), (1, at.prv), (2, at.far)):
            arrival(pc.at[chip], pass_s.at[k], pass_r.at[k], at.partner).wait_send()
        for copy in outs:
            copy.wait()

    late = n_chunks - early
    pl.run_scoped(
        feed,
        V((late, dim, chunk), BF16), V((late + 1, chunk, dim), BF16), V((rows, dim), BF16), V((small, dim), F32),
        V((2, small, chunk), BF16))


def layer(sp, x, wq, wk, wv, wo, wu, wd, rel, gp, chunk=768, early=5):
    rows, dim = x.shape
    heads, head = wq.shape[1:]
    width = (rel.shape[1] - 1) // 2
    ext = rows + 2 * width
    n_glob = gp.shape[1]
    share, chips = n_glob // sp, sp // 2
    cols = heads * share
    n_chunks = wu.shape[1] // chunk
    small = (rows + share) // 3
    anyspec = pl.BlockSpec(memory_space=pl.ANY)
    vmem = pl.BlockSpec(memory_space=pltpu.VMEM)
    dma = pltpu.SemaphoreType.DMA
    V = pltpu.VMEM
    return pl.pallas_call(
        functools.partial(layer_kernel, sp, chunk, small),
        out_shape=(jax.ShapeDtypeStruct((rows, dim), BF16), jax.ShapeDtypeStruct((sp, share, dim), BF16)),
        in_specs=[anyspec] * 7 + [vmem] * 2,
        out_specs=(anyspec, anyspec),
        scratch_shapes=[
            V(x.shape, BF16), V(wo.shape, BF16), V((head, ext), BF16), V((ext, head), BF16),
            V((chips, share, dim), BF16), V((chips, share, dim), BF16), V((chips, share, dim), BF16),
            V((chips - 1, share, dim), BF16), V((sp, share, dim), BF16),
            V((sp, head + 8, cols), F32), V((chips, head + 8, cols), F32), V((3, head + 8, cols), F32),
            V((rows + share, dim), BF16), V((sp, share, dim), BF16),
            V((early, dim, chunk), BF16), V((early - 1, chunk, dim), BF16),
            dma((5,)), dma((4,)), dma((n_chunks,)), dma((n_chunks,)),
            dma((4,)), dma((4,)), dma((4,)), dma((4,)), dma((7,)), dma((7,)), dma((1,)), dma((1,)), dma((3,)), dma((3,)),
            dma((7,)), dma((7,)),
        ],
        compiler_params=pltpu.CompilerParams(
            collective_id=0, has_side_effects=True, vmem_limit_bytes=VMEM_LIMIT),
        name='layer',
    )(x, wq, wk, wv, wo, wu, wd, rel, gp)


def gelu(z):
    c = (2.0 / jnp.pi) ** 0.5
    hz = 0.5 * z
    return (hz + hz * jnp.tanh(z * (c + (c * 0.044715) * (z * z)))).astype(BF16)


def place_kernel(y_ref, yg_ref, gp_ref, out_ref, outg_ref):
    n, n_glob = y_ref.shape[0], gp_ref.shape[1]
    first = lax.axis_index('sp') * n * pl.num_programs(0) + pl.program_id(0) * n
    pos = first + lax.broadcasted_iota(jnp.int32, (n, n_glob), 0)
    hit = jnp.where(pos == gp_ref[...], 1.0, 0.0)
    here = jnp.sum(hit, axis=1, keepdims=True) > 0.5
    out_ref[...] = jnp.where(here, mm(hit.astype(BF16), yg_ref[...]).astype(BF16), y_ref[...])
    outg_ref[...] = yg_ref[...]


def place(y, y_glob, gp, steps=2):
    rows, dim = y.shape
    n = rows // steps
    whole = pl.BlockSpec(y_glob.shape, lambda i: (0, 0))
    return pl.pallas_call(
        place_kernel,
        grid=(steps,),
        out_shape=(jax.ShapeDtypeStruct(y.shape, BF16), jax.ShapeDtypeStruct(y_glob.shape, BF16)),
        in_specs=[pl.BlockSpec((n, dim), lambda i: (i, 0)), whole, pl.BlockSpec(gp.shape, lambda i: (0, 0))],
        out_specs=(pl.BlockSpec((n, dim), lambda i: (i, 0)), whole),
        name='place',
    )(y, y_glob, gp)


def solution(mesh):
    sp = mesh.shape['sp']

    def shard_layer(hidden_in, w_query, w_key, w_value, w_out, w_up, w_down, rel_bias, glob_pos):
        dim = hidden_in.shape[1]
        heads, head = w_query.shape[1], w_query.shape[2]
        gp = glob_pos[None, :]
        wo = w_out.reshape(heads * head, dim)
        y, y_glob = layer(
            sp, hidden_in, w_query, w_key.reshape(dim, head), w_value.reshape(dim, head), wo, w_up, w_down, rel_bias, gp)
        return place(y, y_glob.reshape(-1, dim), gp)

    return jax.shard_map(
        shard_layer, mesh=mesh,
        in_specs=(P(('dp', 'sp'), None), P(), P(), P(), P(), P(), P(), P(), P('dp')),
        out_specs=(P(('dp', 'sp'), None), P('dp', None)),
        check_vma=False)
```

```python
import functools

import jax
import jax.numpy as jnp
from jax import lax
from jax.experimental import pallas as pl
from jax.experimental.pallas import tpu as pltpu
from jax.sharding import PartitionSpec as P

MESH = pl.DeviceIdType.MESH
F32 = jnp.float32
BF16 = jnp.bfloat16
QB = 128
VMEM_LIMIT = 60 * 1024 * 1024


def mm(a, b):
    return jnp.dot(a, b, preferred_element_type=F32)


def mm_ta(a, b):
    return lax.dot_general(a, b, (((0,), (0,)), ((), ())), preferred_element_type=F32)


def mm_tb(a, b):
    return lax.dot_general(a, b, (((1,), (1,)), ((), ())), preferred_element_type=F32)


def send(src, dst, ssem, rsem, dev):
    copy = pltpu.make_async_remote_copy(
        src_ref=src, dst_ref=dst, send_sem=ssem, recv_sem=rsem, device_id={'sp': dev}, device_id_type=MESH)
    copy.start()
    return copy


def arrival(ref, ssem, rsem, dev):
    return pltpu.make_async_remote_copy(
        src_ref=ref, dst_ref=ref, send_sem=ssem, recv_sem=rsem, device_id={'sp': dev}, device_id_type=MESH)


def greet(sp):
    me = lax.axis_index('sp')
    barrier = pltpu.get_barrier_semaphore()
    for k in range(1, sp):
        pl.semaphore_signal(barrier, inc=1, device_id={'sp': lax.rem(me + k, sp)}, device_id_type=MESH)
    return barrier


class Place:
    def __init__(self, sp):
        me = lax.axis_index('sp')
        chips = sp // 2
        assert chips == 4
        self.me, self.chips = me, chips
        self.chip, self.core = me // 2, lax.rem(me, 2)
        self.nxt = lax.rem(self.chip + 1 - 2 * self.core + chips, chips)
        self.prv = lax.rem(self.chip - 1 + 2 * self.core + chips, chips)
        self.far = lax.rem(self.chip + 2, chips)
        self.to_nxt, self.to_prv = self.nxt * 2 + self.core, self.prv * 2 + self.core
        self.to_far = self.far * 2 + self.core
        self.partner = self.chip * 2 + 1 - self.core
        self.base, self.other = self.core * chips, (1 - self.core) * chips


class Gather:
    def __init__(self, at, buf, ss, rs):
        self.at, self.buf, self.ss, self.rs = at, buf, ss, rs

    def push(self, chip, k, dev):
        ref = self.buf.at[self.at.base + chip]
        send(ref, ref, self.ss.at[k], self.rs.at[k], dev)

    def landed(self, slot, k):
        arrival(self.buf.at[slot], self.ss.at[k], self.rs.at[k], self.at.partner).wait_recv()

    def start(self):
        at = self.at
        self.push(at.chip, 0, at.to_nxt)
        self.push(at.chip, 2, at.to_far)
        self.push(at.chip, 1, at.to_prv)
        self.push(at.chip, 3, at.partner)

    def hop(self):
        at = self.at
        self.landed(at.base + at.prv, 0)
        self.push(at.prv, 4, at.partner)

    def end(self):
        at = self.at
        self.landed(at.base + at.nxt, 1)
        self.push(at.nxt, 5, at.partner)
        self.landed(at.base + at.far, 2)
        self.push(at.far, 6, at.partner)

    def finish(self):
        at = self.at
        for k, chip in ((3, at.chip), (4, at.nxt), (5, at.prv), (6, at.far)):
            self.landed(at.other + chip, k)
        for k, chip in ((0, at.chip), (1, at.chip), (2, at.chip), (3, at.chip), (4, at.prv), (5, at.nxt), (6, at.far)):
            arrival(self.buf.at[at.base + chip], self.ss.at[k], self.rs.at[k], at.partner).wait_send()


def merge(head, blocks):
    best = functools.reduce(jnp.maximum, [v[head : head + 1] for v in blocks])
    num, total = 0.0, 0.0
    for v in blocks:
        f = jnp.exp(v[head : head + 1] - best)
        num = num + v[0:head] * f
        total = total + v[head + 1 : head + 2] * f
    return num, best, total


def pack(ref, slot, head, num, best, total):
    ref[slot, 0:head, :] = num
    ref[slot, head:, :] = jnp.concatenate([best, total, jnp.zeros((6, best.shape[1]), F32)], axis=0)


def layer_kernel(sp, chunk, small, x_hbm, wq_hbm, wk_hbm, wv_hbm, wo_hbm, wu_hbm, wd_hbm, rel_ref, gp_ref, y_hbm, yg_hbm,
                 x_ref, wo_ref, kt, vext, xp, xq, xs, xr, xg, part, pc, pr, hb, gbuf, wu_a, wd_a,
                 load_sem, out_sem, wu_sem, wd_sem, halo_s, halo_r, pick_s, pick_r, xg_s, xg_r, part_s, part_r, pass_s, pass_r, yg_s, yg_r):
    at = Place(sp)
    me, chips = at.me, at.chips
    rows, dim = x_ref.shape
    heads, head = wq_hbm.shape[1:]
    width = (rel_ref.shape[1] - 1) // 2
    span = 2 * width + QB
    n_glob = gp_ref.shape[1]
    share = n_glob // sp
    cols = heads * share
    ext = rows + 2 * width
    seq = rows * sp
    start = me * rows
    blocks = rows // QB
    scale = head ** -0.5
    n_chunks = wu_hbm.shape[1] // chunk
    early = wu_a.shape[0]
    cut = 2 * small - share

    def up_to(c, ref):
        return pltpu.make_async_copy(wu_hbm.at[:, pl.ds(pl.multiple_of(c * chunk, chunk), chunk)], ref, wu_sem.at[c])

    def down_to(c, ref):
        return pltpu.make_async_copy(wd_hbm.at[pl.ds(pl.multiple_of(c * chunk, chunk), chunk), :], ref, wd_sem.at[c])

    early_loads = [up_to(c, wu_a.at[c]) for c in range(early)] + [down_to(c, wd_a.at[c]) for c in range(early - 1)]
    right, left = lax.rem(me + 1, sp), lax.rem(me + sp - 1, sp)
    barrier = greet(sp)

    def attend(wq3, wq_ref, wk_ref, wv_ref, rel_pad, tile, onehot, kmask, kloc, vt, qs, qg, ktg, vg, num_ref, top_ref, sum_ref, att):
        loads = []
        for i, (src, dst) in enumerate(((x_hbm, x_ref), (wk_hbm, wk_ref), (wv_hbm, wv_ref), (wq_hbm, wq3), (wo_hbm, wo_ref))):
            loads.append(pltpu.make_async_copy(src, dst, load_sem.at[i]))
        loads[0].start()
        loads[1].start()

        pos = start - width + lax.broadcasted_iota(jnp.int32, (ext, n_glob), 0)
        onehot[...] = jnp.where(pos == gp_ref[...], 1.0, 0.0).astype(BF16)

        count = mm_tb(jnp.ones((8, n_glob), BF16), onehot[...])[0:1]
        col = start - width + lax.broadcasted_iota(jnp.int32, (1, ext), 1)
        kmask[...] = jnp.where((count > 0.5) | (col < 0) | (col >= seq), -jnp.inf, 0.0)
        rel_pad[...] = jnp.full(rel_pad.shape, -jnp.inf, F32)
        rel_pad[:, : 2 * width + 1] = rel_ref[...]
        for h in range(heads):
            line = jnp.broadcast_to(rel_pad[h : h + 1, :], (QB, span))
            tile[h * QB : (h + 1) * QB, :] = pltpu.roll(line, 0, 1, stride=1, stride_axis=0)

        def pick(rank):
            some = pl.ds(pl.multiple_of(rank * share, QB), chips * share)
            return mm_ta(onehot[width : width + rows, some], x_ref[...]).astype(BF16).reshape(xp.shape)

        loads[0].wait()
        for copy in loads[2:]:
            copy.start()
        xp[...] = pick(at.other)
        pl.semaphore_wait(barrier, sp - 1)
        pick_send = [send(xp, xq, pick_s.at[0], pick_r.at[0], at.partner)]
        xs[...] = pick(at.base)

        def key_rows(lo, hi):
            k32 = mm(x_ref[lo:hi, :], wk_ref[...])
            kloc[lo:hi, :] = k32.astype(BF16)
            kt[:, width + lo : width + hi] = k32.T.astype(BF16)

        loads[1].wait()
        key_rows(0, rows // 2)
        arrival(xq, pick_s.at[0], pick_r.at[0], at.partner).wait_recv()
        xs[...] = xs[...] + xq[...]
        pick_send.append(send(xs.at[at.far], xr.at[2], pick_s.at[2], pick_r.at[2], at.to_nxt))
        pick_send.append(send(xs.at[at.prv], xr.at[1], pick_s.at[1], pick_r.at[1], at.to_prv))
        key_rows(rows // 2, rows)

        loads[2].wait()
        v32 = mm(x_ref[...], wv_ref[...])
        vext[width : width + rows, :] = v32.astype(BF16)
        vt[...] = v32.T.astype(BF16)
        halo = [
            send(kt.at[:, pl.ds(rows, width)], kt.at[:, pl.ds(0, width)], halo_s.at[0], halo_r.at[0], right),
            send(kt.at[:, pl.ds(width, width)], kt.at[:, pl.ds(width + rows, width)], halo_s.at[1], halo_r.at[1], left),
            send(vext.at[pl.ds(rows, width)], vext.at[pl.ds(0, width)], halo_s.at[2], halo_r.at[2], right),
            send(vext.at[pl.ds(width, width)], vext.at[pl.ds(width + rows, width)], halo_s.at[3], halo_r.at[3], left),
        ]

        loads[3].wait()
        wq_ref[...] = wq3[...].reshape(wq_ref.shape)

        def project(b):
            qb = (mm(x_ref[b * QB : (b + 2) * QB, :], wq_ref[...]) * scale).astype(BF16)
            for r in range(2):
                for h in range(heads):
                    qs[b + r, h * QB : (h + 1) * QB, :] = qb[r * QB : (r + 1) * QB, h * head : (h + 1) * head]

        project(0)
        arrival(xr.at[2], pick_s.at[2], pick_r.at[2], at.partner).wait_recv()
        xs[at.nxt] = xs[at.nxt] + xr[2]
        pick_send.append(send(xs.at[at.nxt], xr.at[0], pick_s.at[3], pick_r.at[3], at.to_nxt))
        for b in range(2, blocks, 2):
            project(b)

        arrival(xr.at[0], pick_s.at[3], pick_r.at[3], at.partner).wait_recv()
        arrival(xr.at[1], pick_s.at[1], pick_r.at[1], at.partner).wait_recv()
        xg[at.base + at.chip] = xs[at.chip] + xr[0] + xr[1]
        gather = Gather(at, xg, xg_s, xg_r)
        gather.start()
        loads[4].wait()
        for copy in early_loads:
            copy.start()

        def window(b):
            lo = max(b * QB, width)
            hi = b * QB + span if b >= blocks // 2 else min(b * QB + span, width + rows)
            s = mm(qs[b], kt[:, lo:hi]) + tile[:, lo - b * QB : hi - b * QB] + kmask[:, lo:hi]
            top = jnp.max(s, axis=1, keepdims=True)
            e = jnp.exp(s - top)
            total = jnp.sum(e, axis=1, keepdims=True)
            num_ref[b] = mm(e.astype(BF16), vext[lo:hi, :])
            top_ref[b] = jnp.broadcast_to(top, top_ref.shape[1:])
            sum_ref[b] = jnp.broadcast_to(total, sum_ref.shape[1:])

        for b in range(blocks // 2):
            window(b)
        gather.hop()
        for copy in halo:
            copy.wait_recv()
        for b in range(blocks // 2, blocks):
            window(b)
        gather.end()

        def global_rows(rank):
            some = pl.ds(pl.multiple_of(rank * share, QB), chips * share)
            xgv = xg[pl.ds(rank, chips)].reshape(chips * share, dim)
            ktg[:, some] = mm(xgv, wk_ref[...]).T.astype(BF16)
            vg[some, :] = mm(xgv, wv_ref[...]).astype(BF16)
            qgv = (mm(xgv, wq_ref[...]) * scale).astype(BF16)
            for r in range(chips):
                for h in range(heads):
                    qg[r, h * share : (h + 1) * share, :] = qgv[r * share : (r + 1) * share, h * head : (h + 1) * head]
            for c in range(0, chips, 2):
                s = mm_tb(kloc[...], qg[c : c + 2].reshape(2 * cols, head))
                top = jnp.max(s, axis=0, keepdims=True)
                e = jnp.exp(s - top)
                total = jnp.sum(e, axis=0, keepdims=True)
                num = mm(vt[...], e.astype(BF16))
                for r in range(2):
                    here = slice(r * cols, (r + 1) * cols)
                    pack(part, rank + c + r, head, num[:, here], top[:, here], total[:, here])

        def parity(i, carry):
            @pl.when(i == 1)
            def _():
                gather.finish()

            global_rows(lax.rem(at.core + i, 2) * chips)
            return carry

        lax.fori_loop(0, 2, parity, 0)
        part_send = send(part.at[pl.ds(at.other, chips)], pc, part_s.at[0], part_r.at[0], at.partner)

        def complete(b):
            lo, hi = b * QB, max(b * QB, width)
            scores = [(mm(qs[b], ktg[...]), vg[...])]
            if lo < hi:
                s = mm(qs[b], kt[:, lo:hi]) + tile[:, : hi - lo] + kmask[:, lo:hi]
                scores.append((s, vext[lo:hi, :]))
            if b >= blocks // 2:
                scores = scores[:1]
            top = top_ref[b]
            best = top
            for s, _ in scores:
                best = jnp.maximum(best, jnp.max(s, axis=1, keepdims=True))
            fade = jnp.exp(top - best)
            o, sums = 0.0, 0.0
            for s, v in scores:
                e = [jnp.exp(s[:, i : i + QB] - best) for i in range(0, s.shape[1], QB)]
                sums = sums + functools.reduce(jnp.add, e)
                o = o + mm(jnp.concatenate(e, axis=1).astype(BF16), v)
            inv = 1.0 / (sum_ref[b] * fade + jnp.sum(sums, axis=1, keepdims=True))
            o = jnp.concatenate(
                [((num_ref[b, :, i : i + QB] * fade + o[:, i : i + QB]) * inv).astype(BF16) for i in range(0, head, QB)], axis=1)
            for h in range(heads):
                att[b * QB : (b + 1) * QB, h * head : (h + 1) * head] = o[h * QB : (h + 1) * QB]

        for b in range(blocks):
            complete(b)

        arrival(pc, part_s.at[0], part_r.at[0], at.partner).wait_recv()
        for c in range(chips):
            pack(pc, c, head, *merge(head, [part[at.base + c], pc[c]]))
        send(pc.at[at.far], pr.at[2], pass_s.at[2], pass_r.at[2], at.to_nxt)
        send(pc.at[at.prv], pr.at[1], pass_s.at[1], pass_r.at[1], at.to_prv)

        for b in range(0, blocks, 2):
            lo, hi = b * QB, (b + 2) * QB
            v = (x_ref[lo:hi, :].astype(F32) + mm(att[lo:hi, :], wo_ref[...])).astype(BF16)
            mid = min(max(cut, lo), hi)
            if lo < mid:
                hb[lo:mid, :] = v[: mid - lo]
            if mid < hi:
                hb[mid + share : hi + share, :] = v[mid - lo :]
        for copy in halo + pick_send + [part_send]:
            copy.wait_send()

    V = pltpu.VMEM
    pl.run_scoped(
        attend,
        V(wq_hbm.shape, BF16), V((dim, heads * head), BF16), V(wk_hbm.shape, BF16), V(wv_hbm.shape, BF16),
        V((heads, span), F32), V((heads * QB, span), F32), V((ext, n_glob), BF16), V((1, ext), F32),
        V((rows, head), BF16), V((head, rows), BF16), V((blocks, heads * QB, head), BF16), V((chips, cols, head), BF16),
        V((head, n_glob), BF16), V((n_glob, head), BF16),
        V((blocks, heads * QB, head), F32), V((blocks, heads * QB, QB), F32), V((blocks, heads * QB, QB), F32),
        V((rows, heads * head), BF16))

    def feed(wu_b, wd_b, ybuf, acc, ubuf):
        late_loads = [down_to(early - 1, wd_b.at[0])]
        for c in range(early, n_chunks):
            late_loads += [up_to(c, wu_b.at[c - early]), down_to(c, wd_b.at[c - early + 1])]
        for copy in late_loads:
            copy.start()

        arrival(pr.at[2], pass_s.at[2], pass_r.at[2], at.partner).wait_recv()
        pack(pc, at.nxt, head, *merge(head, [pc[at.nxt], pr[2]]))
        send(pc.at[at.nxt], pr.at[0], pass_s.at[0], pass_r.at[0], at.to_nxt)
        for copy in early_loads:
            copy.wait()

        gather = Gather(at, gbuf, yg_s, yg_r)
        ends = (0, small, 2 * small - share, rows)
        outs = [
            pltpu.make_async_copy(ybuf.at[pl.ds(a, b - a)], y_hbm.at[pl.ds(a, b - a)], out_sem.at[p])
            for p, (a, b) in enumerate(zip(ends[:-1], ends[1:]))]

        def one_tile(p, carry):
            here = pl.ds(pl.multiple_of(p * small, share), small)
            acc[...] = hb[here, :].astype(F32)
            for c in range(early):
                ubuf[c % 2] = gelu(mm(hb[here, :], wu_a[c]))
                if c:
                    acc[...] += mm(ubuf[(c - 1) % 2], wd_a[c - 1])

            @pl.when(p == 0)
            def _():
                for copy in late_loads:
                    copy.wait()
                for k in range(2):
                    arrival(pr.at[k], pass_s.at[k], pass_r.at[k], at.partner).wait_recv()
                num, best, total = merge(head, [pc[at.chip], pr[0], pr[1]])
                og = (num / total).T.astype(BF16)
                ag = jnp.concatenate([og[h * share : (h + 1) * share] for h in range(heads)], axis=1)
                hb[cut : cut + share, :] = (xg[at.base + at.chip].astype(F32) + mm(ag, wo_ref[...])).astype(BF16)

            @pl.when(p == 2)
            def _():
                gather.hop()
                gather.end()

            for c in range(early, n_chunks):
                ubuf[c % 2] = gelu(mm(hb[here, :], wu_b[c - early]))
                acc[...] += mm(ubuf[(c - 1) % 2], wd_b[c - early])
            y = (acc[...] + mm(ubuf[(n_chunks - 1) % 2], wd_b[n_chunks - early])).astype(BF16)

            @pl.when(p == 0)
            def _():
                ybuf[0:small, :] = y
                outs[0].start()

            @pl.when(p == 1)
            def _():
                ybuf[small:cut, :] = y[0 : small - share]
                gbuf[at.base + at.chip] = y[small - share :]
                gather.start()
                outs[1].start()

            @pl.when(p == 2)
            def _():
                ybuf[cut:rows, :] = y
                outs[2].start()

            return carry

        lax.fori_loop(0, 3, one_tile, 0)
        gather.finish()
        outs.append(pltpu.make_async_copy(gbuf, yg_hbm, out_sem.at[3]))
        outs[3].start()
        for k, chip in ((0, at.nxt), (1, at.prv), (2, at.far)):
            arrival(pc.at[chip], pass_s.at[k], pass_r.at[k], at.partner).wait_send()
        for copy in outs:
            copy.wait()

    late = n_chunks - early
    pl.run_scoped(
        feed,
        V((late, dim, chunk), BF16), V((late + 1, chunk, dim), BF16), V((rows, dim), BF16), V((small, dim), F32),
        V((2, small, chunk), BF16))


def layer(sp, x, wq, wk, wv, wo, wu, wd, rel, gp, chunk=768, early=5):
    rows, dim = x.shape
    heads, head = wq.shape[1:]
    width = (rel.shape[1] - 1) // 2
    ext = rows + 2 * width
    n_glob = gp.shape[1]
    share, chips = n_glob // sp, sp // 2
    cols = heads * share
    n_chunks = wu.shape[1] // chunk
    small = (rows + share) // 3
    anyspec = pl.BlockSpec(memory_space=pl.ANY)
    vmem = pl.BlockSpec(memory_space=pltpu.VMEM)
    dma = pltpu.SemaphoreType.DMA
    V = pltpu.VMEM
    return pl.pallas_call(
        functools.partial(layer_kernel, sp, chunk, small),
        out_shape=(jax.ShapeDtypeStruct((rows, dim), BF16), jax.ShapeDtypeStruct((sp, share, dim), BF16)),
        in_specs=[anyspec] * 7 + [vmem] * 2,
        out_specs=(anyspec, anyspec),
        scratch_shapes=[
            V(x.shape, BF16), V(wo.shape, BF16), V((head, ext), BF16), V((ext, head), BF16),
            V((chips, share, dim), BF16), V((chips, share, dim), BF16), V((chips, share, dim), BF16),
            V((chips - 1, share, dim), BF16), V((sp, share, dim), BF16),
            V((sp, head + 8, cols), F32), V((chips, head + 8, cols), F32), V((3, head + 8, cols), F32),
            V((rows + share, dim), BF16), V((sp, share, dim), BF16),
            V((early, dim, chunk), BF16), V((early - 1, chunk, dim), BF16),
            dma((5,)), dma((4,)), dma((n_chunks,)), dma((n_chunks,)),
            dma((4,)), dma((4,)), dma((4,)), dma((4,)), dma((7,)), dma((7,)), dma((1,)), dma((1,)), dma((3,)), dma((3,)),
            dma((7,)), dma((7,)),
        ],
        compiler_params=pltpu.CompilerParams(
            collective_id=0, has_side_effects=True, vmem_limit_bytes=VMEM_LIMIT),
        name='layer',
    )(x, wq, wk, wv, wo, wu, wd, rel, gp)


def gelu(z):
    c = (2.0 / jnp.pi) ** 0.5
    hz = 0.5 * z
    return (hz + hz * jnp.tanh(z * (c + (c * 0.044715) * (z * z)))).astype(BF16)


def place_kernel(y_ref, yg_ref, gp_ref, out_ref, outg_ref):
    n, n_glob = y_ref.shape[0], gp_ref.shape[1]
    first = lax.axis_index('sp') * n * pl.num_programs(0) + pl.program_id(0) * n
    pos = first + lax.broadcasted_iota(jnp.int32, (n, n_glob), 0)
    hit = jnp.where(pos == gp_ref[...], 1.0, 0.0)
    here = jnp.sum(hit, axis=1, keepdims=True) > 0.5
    out_ref[...] = jnp.where(here, mm(hit.astype(BF16), yg_ref[...]).astype(BF16), y_ref[...])
    outg_ref[...] = yg_ref[...]


def place(y, y_glob, gp, steps=2):
    rows, dim = y.shape
    n = rows // steps
    whole = pl.BlockSpec(y_glob.shape, lambda i: (0, 0))
    return pl.pallas_call(
        place_kernel,
        grid=(steps,),
        out_shape=(jax.ShapeDtypeStruct(y.shape, BF16), jax.ShapeDtypeStruct(y_glob.shape, BF16)),
        in_specs=[pl.BlockSpec((n, dim), lambda i: (i, 0)), whole, pl.BlockSpec(gp.shape, lambda i: (0, 0))],
        out_specs=(pl.BlockSpec((n, dim), lambda i: (i, 0)), whole),
        name='place',
    )(y, y_glob, gp)


def solution(mesh):
    sp = mesh.shape['sp']

    def shard_layer(hidden_in, w_query, w_key, w_value, w_out, w_up, w_down, rel_bias, glob_pos):
        dim = hidden_in.shape[1]
        heads, head = w_query.shape[1], w_query.shape[2]
        gp = glob_pos[None, :]
        wo = w_out.reshape(heads * head, dim)
        y, y_glob = layer(
            sp, hidden_in, w_query, w_key.reshape(dim, head), w_value.reshape(dim, head), wo, w_up, w_down, rel_bias, gp)
        return place(y, y_glob.reshape(-1, dim), gp)

    return jax.shard_map(
        shard_layer, mesh=mesh,
        in_specs=(P(('dp', 'sp'), None), P(), P(), P(), P(), P(), P(), P(), P('dp')),
        out_specs=(P(('dp', 'sp'), None), P('dp', None)),
        check_vma=False)
```
